32 devices in a mesh: band: 8 (over z, y), dir: 4 (over x, core).
Axes of the slice: x: 2, y: 2, z: 4, core: 2. Of those that a mesh axis runs over, the one named last changes fastest.
Arguments:
- visibilities: float32 [8, 2, 2, 2, 16, 512], P('band'), may hold values from -6 to 6
- coherencies: float32 [8, 16, 2, 2, 2, 16, 512], P('band', 'dir'), may hold values from -1.2 to 1.2
- jones_start: float32 [8, 16, 2, 2, 2, 1024], P('band', 'dir'), may hold values from -3.6 to 3.6
- dual_start: float32 [8, 16, 2, 2, 2, 1024], P('band', 'dir'), may hold values from -6 to 6
- consensus_start: float32 [8, 16, 2, 2, 2, 1024], P(None, 'dir'), may hold values from -1.8 to 1.8
- freq_basis: float32 [8, 8], P('band'), may hold values from -1 to 1
- baseline_station_pairs: int32 [2, 512], replicated, may hold values from 0 to 1023
Outputs:
- jones_final: float32 [8, 16, 2, 2, 2, 1024], P('band', 'dir')
- dual_final: float32 [8, 16, 2, 2, 2, 1024], P('band', 'dir')
- consensus_coeffs: float32 [8, 16, 2, 2, 2, 1024], P(None, 'dir')
The draws below stay inside these ranges and needn't reach their ends.
All inputs are finite; a program needn't handle non-finite values.
Results may differ from the reference program's by a relative error of at most 0.0003.
Values sent between devices are 32-bit elements; how exact they have to be, the bound alone decides.
A program may use at most 128 MiB of HBM per device.

```python
import jax
import jax.numpy as jnp
from jax import lax

STATION_COUNT = 1024
TERMS = 8
TIMESLOT_COUNT = 16
BASELINE_COUNT = 512
ITERS = 3
DIRECTION_COUNT = 16
SUBBAND_COUNT = 8


def place_ends(drawn, own_key, least, top_value):
    spot = [jax.random.randint(jax.random.fold_in(own_key, axis), (), 0, length) for axis, length in enumerate(drawn.shape)]
    widest = drawn.shape.index(max(drawn.shape))
    neighbour = spot[:widest] + [(spot[widest] + 1) % drawn.shape[widest]] + spot[widest + 1:]
    return drawn.at[tuple(spot)].set(least).at[tuple(neighbour)].set(top_value)


def block_levels(key, shape, cuts, low, high):
    loudness = 1.0
    for position, shards_of in cuts:
        draws = jax.random.uniform(jax.random.fold_in(jax.random.fold_in(key, 6), position), (shards_of,), jnp.float32, low / len(cuts), high / len(cuts))
        loudness = loudness * jnp.repeat(jnp.exp(draws), shape[position] // shards_of).reshape((-1,) + (1,) * (len(shape) - 1 - position))
    return loudness


def normal_values(own_key, shape, scale, bound, pieces=(), held_as=jnp.bfloat16):
    loudness = block_levels(own_key, shape, pieces, -0.22, 0.18) if pieces else 1.0
    array = jax.random.normal(own_key, shape, jnp.float32) * scale * loudness
    return jnp.minimum(jnp.maximum(array, -bound), bound).astype(held_as)


def setup_inputs(seed: int = 0) -> dict:
    key_of = jax.random.split(jax.random.key(seed), 8)
    visibilities = normal_values(key_of[0], (SUBBAND_COUNT, 2, 2, 2, TIMESLOT_COUNT, BASELINE_COUNT), 1.0, 6.0, ((0, 8),), jnp.float32)
    coherencies = normal_values(key_of[1], (SUBBAND_COUNT, DIRECTION_COUNT, 2, 2, 2, TIMESLOT_COUNT, BASELINE_COUNT), 0.2, 1.2, ((0, 8), (1, 4)), jnp.float32)
    jones_start = normal_values(key_of[2], (SUBBAND_COUNT, DIRECTION_COUNT, 2, 2, 2, STATION_COUNT), 0.6, 3.6, ((0, 8), (1, 4)), jnp.float32)
    dual_start = normal_values(key_of[3], (SUBBAND_COUNT, DIRECTION_COUNT, 2, 2, 2, STATION_COUNT), 1.0, 6.0, ((0, 8), (1, 4)), jnp.float32)
    consensus_start = normal_values(key_of[4], (TERMS, DIRECTION_COUNT, 2, 2, 2, STATION_COUNT), 0.3, 1.8, ((1, 4),), jnp.float32)
    freq_basis = jnp.clip(jax.random.uniform(key_of[5], (SUBBAND_COUNT, TERMS), jnp.float32, -1.0, 1.0) * block_levels(key_of[5], (SUBBAND_COUNT, TERMS), ((0, 8),), -0.4, 0.0), -1.0, 1.0)
    baseline_station_pairs = place_ends(jax.random.randint(key_of[6], (2, BASELINE_COUNT), 0, STATION_COUNT), jax.random.fold_in(key_of[6], 1), 0, STATION_COUNT - 1).astype(jnp.int32)
    return dict(visibilities=visibilities, coherencies=coherencies, jones_start=jones_start, dual_start=dual_start, consensus_start=consensus_start, freq_basis=freq_basis, baseline_station_pairs=baseline_station_pairs)


RHO = 5.0
RIDGE = 0.25

def small_mul(left, right):
    return left[:, 0:1] * right[0:1] + left[:, 1:2] * right[1:2]

def complex_mul(left, right):
    real_part = small_mul(left[0], right[0]) - small_mul(left[1], right[1])
    imag_part = small_mul(left[0], right[1]) + small_mul(left[1], right[0])
    return jnp.stack([real_part, imag_part])

def hermitian(value):
    return jnp.stack([jnp.swapaxes(value[0], 0, 1), -jnp.swapaxes(value[1], 0, 1)])

def solve_right(numer, matrix):
    adjugate = jnp.stack([jnp.stack([matrix[:, 1, 1], -matrix[:, 0, 1]], axis=1), jnp.stack([-matrix[:, 1, 0], matrix[:, 0, 0]], axis=1)], axis=1)
    det_real = matrix[0, 0, 0] * matrix[0, 1, 1] - matrix[1, 0, 0] * matrix[1, 1, 1] - (matrix[0, 0, 1] * matrix[0, 1, 0] - matrix[1, 0, 1] * matrix[1, 1, 0])
    det_imag = matrix[0, 0, 0] * matrix[1, 1, 1] + matrix[1, 0, 0] * matrix[0, 1, 1] - (matrix[0, 0, 1] * matrix[1, 1, 0] + matrix[1, 0, 1] * matrix[0, 1, 0])
    product = complex_mul(numer, adjugate)
    divisor = det_real * det_real + det_imag * det_imag
    real_part = (product[0] * det_real + product[1] * det_imag) / divisor
    imag_part = (product[1] * det_real - product[0] * det_imag) / divisor
    return jnp.stack([real_part, imag_part])

def predict(jones_k, coher_k, first, second):
    jones_first = jnp.take(jones_k, first, axis=-1)[..., None, :]
    jones_second = jnp.take(jones_k, second, axis=-1)[..., None, :]
    return complex_mul(complex_mul(jones_first, coher_k), hermitian(jones_second))

def baseline_terms(target, jones_k, coher_k, first, second):
    jones_first = jnp.take(jones_k, first, axis=-1)[..., None, :]
    jones_second = jnp.take(jones_k, second, axis=-1)[..., None, :]
    along_term = complex_mul(coher_k, hermitian(jones_second))
    back_term = hermitian(complex_mul(jones_first, coher_k))
    flipped = hermitian(target)
    right_first = jnp.sum(complex_mul(target, hermitian(along_term)), axis=-2)
    normal_first = jnp.sum(complex_mul(along_term, hermitian(along_term)), axis=-2)
    right_second = jnp.sum(complex_mul(flipped, hermitian(back_term)), axis=-2)
    normal_second = jnp.sum(complex_mul(back_term, hermitian(back_term)), axis=-2)
    first_part = jnp.concatenate([right_first.reshape(8, -1), normal_first.reshape(8, -1)], axis=0)
    second_part = jnp.concatenate([right_second.reshape(8, -1), normal_second.reshape(8, -1)], axis=0)
    return jnp.concatenate([first_part, second_part], axis=1)

def update_one(right_sum, normal_sum, consensus, dual):
    identity = jnp.stack([jnp.eye(2, dtype=jnp.float32), jnp.zeros((2, 2), jnp.float32)])[..., None]
    matrix = normal_sum + RHO * identity
    return solve_right(right_sum + RHO * consensus - dual, matrix)

def update_band(band_items, first, second):
    vis, coher, jones, dual, consensus = band_items
    stations = jones.shape[-1]
    dirs = jones.shape[0]
    model_terms = jax.vmap(predict, (0, 0, None, None))(jones, coher, first, second)
    residual = vis - jnp.sum(model_terms, axis=0)
    normal_terms = jax.vmap(baseline_terms, (0, 0, 0, None, None))(residual[None] + model_terms, jones, coher, first, second)
    stacked = normal_terms.reshape(dirs * 16, -1)
    segment_ids = jnp.concatenate([first, second]).astype(jnp.int32)
    segment = jax.ops.segment_sum(stacked.T, segment_ids, num_segments=stations).T
    segment = segment.reshape((dirs, 2, 2, 2, 2, stations))
    return jax.vmap(update_one)(segment[:, 0], segment[:, 1], consensus, dual)

def reference(visibilities, coherencies, jones_start, dual_start, consensus_start, freq_basis, baseline_station_pairs):
    first = baseline_station_pairs[0]
    second = baseline_station_pairs[1]
    terms = freq_basis.shape[1]
    gram = jnp.dot(freq_basis.T, freq_basis, precision=lax.Precision.HIGHEST) + RIDGE * freq_basis.shape[0] * jnp.eye(terms, dtype=jnp.float32)
    scale_factor = jnp.linalg.cholesky(gram)
    jones = jones_start
    dual = dual_start
    coeffs = consensus_start
    consensus = jnp.einsum('fm,mkabcs->fkabcs', freq_basis, coeffs, precision=lax.Precision.HIGHEST)
    for turn_index in range(ITERS):
        jones = lax.map(lambda band_items: update_band(band_items, first, second), (visibilities, coherencies, jones, dual, consensus))
        coeff_sums = jnp.einsum('fm,fkabcs->mkabcs', freq_basis, jones + dual / RHO, precision=lax.Precision.HIGHEST)
        flat = coeff_sums.reshape(terms, -1)
        coeffs = jax.scipy.linalg.cho_solve((scale_factor, True), flat).reshape(coeff_sums.shape)
        consensus = jnp.einsum('fm,mkabcs->fkabcs', freq_basis, coeffs, precision=lax.Precision.HIGHEST)
        dual = dual + RHO * (jones - consensus)
    return (jones, dual, coeffs)
```

```python
import functools

import jax
import jax.numpy as jnp
from jax import lax
from jax.experimental import pallas as pl
from jax.experimental.pallas import tpu as pltpu
from jax.sharding import PartitionSpec as P

ITERS = 3
RHO = 5.0
RIDGE = 0.25
LANES = 128
SUB = 8
PIECES = 3
ANSWER = 1
MESH = pl.DeviceIdType.MESH


def cmul(a, b):
    return (a[0] * b[0] - a[1] * b[1], a[0] * b[1] + a[1] * b[0])


def cmul_conj(a, b):
    return (a[0] * b[0] + a[1] * b[1], a[1] * b[0] - a[0] * b[1])


def cadd(a, b):
    return (a[0] + b[0], a[1] + b[1])


def conj(a):
    return (a[0], -a[1])


def re_mul(a, b):
    return a[0] * b[0] - a[1] * b[1]


def scale(r, a):
    return (r * a[0], r * a[1])


def split_store(ref, rows, value):
    left = value
    for piece in range(PIECES):
        part = left.astype(jnp.bfloat16)
        ref[piece * rows : (piece + 1) * rows, :] = part
        if piece + 1 < PIECES:
            left = left - part.astype(jnp.float32)


def join(value, rows):
    total = value[0:rows]
    for piece in range(1, PIECES):
        total = total + value[piece * rows : (piece + 1) * rows]
    return total


def kernel(
    n_band, n_dir, dirs, times, base, stations,
    vis_far, coh_far, jones0_far, dual0_far, coeffs0_far, basis_far, pairs_far,
    jones_out, dual_out, coeffs,
    vis, coh, jones0, dual0, coeffs0, basis, pairs_ref,
    jones, dual, row, ids_col,
    cons, xall, rows_all, weights, gweights, wmat,
    xs, inbox, outbox, consin,
    gather_hot, scatter_hot, lhs, lhs_c, lhs_n, ends, grams, cross, vals, vals_n, found, seg, seg_n,
    model, got_a, sums, got_b, got_c, res,
    load_sem, row_send, row_recv, p_send, p_recv, x_send, x_recv, d_send, d_recv,
):
    f32 = jnp.float32
    nrow = 8 * dirs
    per = stations // LANES
    me = lax.axis_index("band")
    mine = lax.axis_index("dir")
    chunks = base // LANES
    halves = times // SUB
    stages = n_dir.bit_length() - 1
    part_rows = nrow * per // n_band
    exchange = by_chunks(n_band, nrow * per)

    def at(pos):
        half = pos // (n_band // 2)
        return (1 - half) * (2 * pos) + half * (2 * (n_band - 1 - pos) + 1)

    odd = lax.rem(me, 2)
    pos = (1 - odd) * (me // 2) + odd * (n_band - 1 - me // 2)
    nexts = (at(lax.rem(pos + 1, n_band)), at(lax.rem(pos + n_band - 1, n_band)))

    def flip_bits(index, mask):
        out = index
        for b in range(mask.bit_length()):
            if mask >> b & 1:
                out = out + (1 - 2 * lax.rem(index // (1 << b), 2)) * (1 << b)
        return out

    def to_of(step):
        return flip_bits(me, step) if power_of_two(n_band) else lax.rem(me + step, n_band)

    def from_of(step):
        return flip_bits(me, step) if power_of_two(n_band) else lax.rem(me + n_band - step, n_band)

    def flip(stage):
        return flip_bits(mine, 1 << stage)

    def drain(ref, sem):
        pltpu.make_async_copy(ref, ref, sem).wait()

    own = lax.rem(mine, 2)
    other = 1 - own

    loads = {}
    for n, (name, source_ref, near) in enumerate((
        ("pairs", pairs_far, pairs_ref),
        ("jones", jones0_far, jones0),
        ("coh", coh_far, coh),
        ("basis", basis_far, basis),
        ("vis", vis_far, vis),
        ("dual", dual0_far, dual0),
        ("coeffs", coeffs0_far, coeffs0),
    )):
        loads[name] = pltpu.make_async_copy(source_ref, near, load_sem.at[n])
        loads[name].start()

    barrier = pltpu.get_barrier_semaphore()
    for step in range(1, n_band):
        pl.semaphore_signal(barrier, inc=1, device_id={"band": to_of(step)}, device_id_type=MESH)
    for stage in range(stages):
        pl.semaphore_signal(barrier, inc=1, device_id={"dir": flip(stage)}, device_id_type=MESH)

    def halves_of(k, v):
        return (k, v // 2, pl.ds(v % 2, per, stride=2), slice(None))

    def packed(k, v):
        return pl.ds((v * dirs + k) * per, per)

    def block_of(j):
        return j % 2, (j // 2) * LANES

    step_rows = 32

    def hot_body(i, carry):
        start = pl.multiple_of(i * step_rows, step_rows)
        for j in range(2 * chunks):
            lane = slice(j * LANES, (j + 1) * LANES)
            sid = lax.broadcasted_iota(jnp.int32, (step_rows, LANES), 0) + i * step_rows
            which, low = block_of(j)
            ids = pairs_ref[which : which + 1, low : low + LANES]
            same = sid == jnp.broadcast_to(ids, (step_rows, LANES))
            gather_hot[pl.ds(start, step_rows), lane] = jnp.where(same, 1.0, 0.0).astype(jnp.bfloat16)
        return carry

    loads["pairs"].wait()
    lax.fori_loop(0, stations // step_rows, hot_body, 0)

    loads["jones"].wait()
    for k in range(dirs):
        for v in range(8):
            jones[packed(k, v), :] = jones0[halves_of(k, v)]

    def scatter_setup():
        for j in range(2 * chunks):
            which, low = block_of(j)
            ids = jnp.broadcast_to(pairs_ref[which : which + 1, low : low + LANES], (LANES, LANES))
            ids_col[j * LANES : (j + 1) * LANES, :] = jnp.transpose(ids)

        def hot_body2(i, carry):
            start = pl.multiple_of(i * step_rows, step_rows)
            col = ids_col[pl.ds(start, step_rows), :]
            for j in range(stations // LANES):
                lane = slice(j * LANES, (j + 1) * LANES)
                sid = lax.broadcasted_iota(jnp.int32, (step_rows, LANES), 1) + j * LANES
                scatter_hot[pl.ds(start, step_rows), lane] = jnp.where(sid == col, 1.0, 0.0).astype(jnp.bfloat16)
            return carry

        lax.fori_loop(0, 2 * base // step_rows, hot_body2, 0)

    def first_sends():
        pl.semaphore_wait(barrier, n_band - 1 + stages)
        loads["basis"].wait()
        row[...] = jnp.zeros((SUB, LANES), f32)
        for m in range(SUB):
            row[m : m + 1, :] = jnp.full((1, LANES), basis[0, m], f32)
        for step in range(1, n_band):
            pltpu.make_async_remote_copy(
                src_ref=row,
                dst_ref=rows_all.at[step],
                send_sem=row_send.at[0],
                recv_sem=row_recv.at[0],
                device_id={"band": to_of(step)},
                device_id_type=MESH,
            ).start()

    pairs = [(a, b) for a in range(4) for b in range(a, 4)]

    def gram_body(j, carry):
        lane = pl.ds(pl.multiple_of(j * LANES, LANES), LANES)
        for k in range(dirs):
            c = [
                [coh[k, v, h * SUB : (h + 1) * SUB, lane] for h in range(halves)]
                for v in range(8)
            ]
            for n, (a, b) in enumerate(pairs):
                real = sum(c[a][h] * c[b][h] + c[4 + a][h] * c[4 + b][h] for h in range(halves))
                grams[(2 * n) * dirs + k : (2 * n) * dirs + k + 1, lane] = jnp.sum(real, axis=0, keepdims=True)
                if a != b:
                    imag = sum(c[4 + a][h] * c[b][h] - c[a][h] * c[4 + b][h] for h in range(halves))
                    grams[(2 * n + 1) * dirs + k : (2 * n + 1) * dirs + k + 1, lane] = jnp.sum(
                        imag, axis=0, keepdims=True
                    )
        return carry

    def start_consensus():
        loads["coeffs"].wait()
        loads["dual"].wait()
        for k in range(dirs):
            for v in range(8):
                dual[packed(k, v), :] = dual0[halves_of(k, v)]
                total = basis[0, 0] * coeffs0[(0,) + halves_of(k, v)]
                for m in range(1, SUB):
                    total = total + basis[0, m] * coeffs0[(m,) + halves_of(k, v)]
                cons[packed(k, v), :] = total

    def solve_weights():
        drain(rows_all.at[pl.ds(1, n_band - 1)], row_recv.at[0])
        rows_all[0] = row[...]
        held = [rows_all[s] for s in range(n_band)]
        columns = []
        for m in range(SUB):
            total = held[0] * held[0][m : m + 1, :]
            for s in range(1, n_band):
                total = total + held[s] * held[s][m : m + 1, :]
            ident = jnp.where(lax.broadcasted_iota(jnp.int32, (SUB, LANES), 0) == m, RIDGE * n_band, 0.0)
            columns.append(total + ident.astype(f32))
        right = list(held)
        iota = lax.broadcasted_iota(jnp.int32, (SUB, LANES), 0)
        for i in range(SUB):
            inverse = 1.0 / columns[i][i : i + 1, :]
            factor = columns[i]
            for group in (columns, right):
                for c in range(len(group)):
                    lead = jnp.broadcast_to(group[c][i : i + 1, :] * inverse, (SUB, LANES))
                    group[c] = jnp.where(iota == i, lead, group[c] - factor * lead)

        def weight_of(a, b):
            return jnp.broadcast_to(jnp.sum(right[b] * held[a], axis=0, keepdims=True), (SUB, LANES))

        for s in range(n_band):
            band = from_of(s)
            gweights[band] = right[s]
            weights[band] = weight_of(0, s)
        if exchange:
            for a in range(n_band):
                for b in range(n_band):
                    wmat[a * n_band + b] = weight_of(a, b)

    x_copies = [{} for _ in range(ITERS)]
    ahead = n_band // 2
    behind = n_band - 1 - ahead

    def ring(turn):
        return 0 if exchange else turn

    def slot_of(way, distance):
        if distance > behind:
            return n_band - 1
        return distance + way * behind if distance else 0

    def reach_of(k, way):
        return ahead if way == k % 2 else behind

    def send_x(turn, k, way, distance):
        to = slot_of(way, distance + 1)
        copy = pltpu.make_async_remote_copy(
            src_ref=xall.at[ring(turn), k, slot_of(way, distance)],
            dst_ref=xall.at[ring(turn), k, to],
            send_sem=x_send.at[0],
            recv_sem=x_recv.at[ring(turn), k, to - 1],
            device_id={"band": nexts[way]},
            device_id_type=MESH,
        )
        copy.start()
        x_copies[turn][(k, way, distance + 1)] = copy

    def pump(turn, distance, chosen=range(dirs)):
        for k in chosen:
            for way in range(2):
                reach = reach_of(k, way)
                if distance <= reach:
                    x_copies[turn][(k, way, distance)].wait_recv()
                    if distance < reach:
                        send_x(turn, k, way, distance)

    def source(slot):
        if slot <= behind:
            return at(lax.rem(pos + n_band - slot, n_band))
        return at(lax.rem(pos + slot - behind, n_band))

    def part_of(k, v):
        here = (v * dirs + k) * per
        return here // part_rows, pl.ds(here % part_rows, per)

    def send_parts(turn):
        for step in range(n_band - 1, 0, -1):
            pltpu.make_async_remote_copy(
                src_ref=xs.at[turn, to_of(step)],
                dst_ref=inbox.at[turn, step],
                send_sem=p_send.at[0],
                recv_sem=p_recv.at[turn, 0],
                device_id={"band": to_of(step)},
                device_id_type=MESH,
            ).start()

    def answer_parts(turn):
        drain(inbox.at[turn, pl.ds(1, n_band - 1)], p_recv.at[turn, 0])
        inbox[turn, 0] = xs[turn, me]
        for a in range(n_band - 1, -1, -1):
            for r in range(part_rows // SUB):
                here = slice(r * SUB, (r + 1) * SUB)
                total = wmat[a * n_band] * inbox[turn, 0, here, :]
                for b in range(1, n_band):
                    total = total + wmat[a * n_band + b] * inbox[turn, b, here, :]
                outbox[turn, a, here, :] = total
            if a:
                pltpu.make_async_remote_copy(
                    src_ref=outbox.at[turn, a],
                    dst_ref=consin.at[turn, me],
                    send_sem=p_send.at[1],
                    recv_sem=p_recv.at[turn, 1],
                    device_id={"band": to_of(a)},
                    device_id_type=MESH,
                ).start()

    def send_d(turn, n, c, src, dst, stage):
        copy = pltpu.make_async_remote_copy(
            src_ref=src,
            dst_ref=dst,
            send_sem=d_send.at[n],
            recv_sem=d_recv.at[turn, n, c],
            device_id={"dir": flip(stage)},
            device_id_type=MESH,
        )
        copy.start()
        return copy

    def end(comp, lane):
        return ends[comp * dirs : (comp + 1) * dirs, lane]

    def gram(a, b, lane):
        if a > b:
            return conj(gram(b, a, lane))
        n = pairs.index((a, b))
        real = grams[(2 * n) * dirs : (2 * n + 1) * dirs, lane]
        if a == b:
            return real
        return (real, grams[(2 * n + 1) * dirs : (2 * n + 2) * dirs, lane])

    def first_of(c):
        return slice(2 * c * LANES, (2 * c + 1) * LANES)

    def second_of(c):
        return slice((2 * c + 1) * LANES, (2 * c + 2) * LANES)

    def chunk_of(c):
        return slice(c * LANES, (c + 1) * LANES)

    for turn in range(ITERS):
        for g in range(nrow // SUB):
            for j in range(per):
                left = jones[pl.ds(g * SUB * per + j, SUB, stride=per), :]
                for piece in range(PIECES):
                    part = left.astype(jnp.bfloat16)
                    lhs[
                        piece * nrow + g * SUB : piece * nrow + (g + 1) * SUB,
                        j * LANES : (j + 1) * LANES,
                    ] = part
                    left = left - part.astype(f32)
        ends[...] = join(jnp.dot(lhs[...], gather_hot[...], preferred_element_type=f32), nrow)

        def predict(c):
            lane, lane_p, lane_q = chunk_of(c), first_of(c), second_of(c)

            def model_body(h, carry):
                time = pl.ds(pl.multiple_of(h * SUB, SUB), SUB)
                total = [None] * 4
                for k in range(dirs):
                    co = [(coh[k, v, time, lane], coh[k, 4 + v, time, lane]) for v in range(4)]

                    def spread(v, where):
                        return tuple(
                            jnp.broadcast_to(
                                ends[(4 * part + v) * dirs + k : (4 * part + v) * dirs + k + 1, where],
                                (SUB, LANES),
                            )
                            for part in range(2)
                        )

                    p = [spread(v, lane_p) for v in range(4)]
                    q = [spread(v, lane_q) for v in range(4)]
                    for a in range(2):
                        b = [cadd(cmul(p[2 * a], co[d]), cmul(p[2 * a + 1], co[2 + d])) for d in range(2)]
                        for d in range(2):
                            term = cadd(cmul_conj(b[0], q[2 * d]), cmul_conj(b[1], q[2 * d + 1]))
                            v = 2 * a + d
                            total[v] = term if total[v] is None else cadd(total[v], term)
                for v in range(4):
                    model[turn, c, 0, v, time, :] = total[v][0]
                    model[turn, c, 1, v, time, :] = total[v][1]
                return carry

            lax.fori_loop(0, halves, model_body, 0)

        if turn == 0:
            loads["coh"].wait()
        hops = []
        for c in range(chunks):
            predict(c)
            if turn == 0 and c == 0:
                first_sends()
            hops.append(send_d(turn, 0, c, model.at[turn, c, other], got_a.at[turn, c], 0))

        def step_first(c):
            hops[c].wait_recv()
            sums[turn, 0, c] = model[turn, c, own] + got_a[turn, c]
            n = 1
            if stages > 1:
                hops[c] = send_d(turn, n, c, sums.at[turn, 0, c], got_b.at[turn, 0, c], 1)
            else:
                share(c)

        def share(c):
            hops[c] = send_d(turn, stages, c, sums.at[turn, stages - 1, c], got_c.at[turn, c], 0)
            lane = chunk_of(c)
            res[own, :, :, lane] = vis[own, :, :, lane] - sums[turn, stages - 1, c]

        def step_next(stage, c):
            hops[c].wait_recv()
            sums[turn, stage, c] = sums[turn, stage - 1, c] + got_b[turn, stage - 1, c]
            if stage + 1 < stages:
                hops[c] = send_d(
                    turn, stage + 1, c, sums.at[turn, stage, c], got_b.at[turn, stage, c], stage + 1
                )
            else:
                share(c)

        def gram_of(j):
            m00 = re_mul(j[0], conj(j[0])) + re_mul(j[2], conj(j[2]))
            m11 = re_mul(j[1], conj(j[1])) + re_mul(j[3], conj(j[3]))
            m01 = cadd(cmul_conj(j[1], j[0]), cmul_conj(j[3], j[2]))
            return m00, m11, m01

        def ends_of(lane):
            return [(end(v, lane), end(4 + v, lane)) for v in range(4)]

        def normals(c):
            lane = chunk_of(c)

            def gr(a, b):
                return gram(a, b, lane)

            jp, jq = ends_of(first_of(c)), ends_of(second_of(c))
            m00, m11, m01 = gram_of(jq)
            p00, p11, p01 = gram_of(jp)
            n1_00 = m00 * gr(0, 0) + m11 * gr(1, 1) + 2.0 * re_mul(m01, gr(0, 1))
            n1_11 = m00 * gr(2, 2) + m11 * gr(3, 3) + 2.0 * re_mul(m01, gr(2, 3))
            n1_01 = cadd(
                cadd(scale(m00, gr(0, 2)), scale(m11, gr(1, 3))),
                cadd(cmul(m01, gr(0, 3)), cmul(conj(m01), gr(1, 2))),
            )
            n2_00 = p00 * gr(0, 0) + p11 * gr(2, 2) + 2.0 * re_mul(p01, gr(2, 0))
            n2_11 = p00 * gr(1, 1) + p11 * gr(3, 3) + 2.0 * re_mul(p01, gr(3, 1))
            n2_01 = cadd(
                cadd(scale(p00, gr(1, 0)), scale(p11, gr(3, 2))),
                cadd(cmul(p01, gr(3, 0)), cmul(conj(p01), gr(1, 2))),
            )
            for n, (left, right) in enumerate(
                ((n1_00, n2_00), (n1_11, n2_11), (n1_01[0], n2_01[0]), (n1_01[1], n2_01[1]))
            ):
                vals_n[n * dirs : (n + 1) * dirs, first_of(c)] = left
                vals_n[n * dirs : (n + 1) * dirs, second_of(c)] = right

        def scatter_normals():
            split_store(lhs_n, 4 * dirs, vals_n[...])
            out = join(jnp.dot(lhs_n[...], scatter_hot[...], preferred_element_type=f32), 4 * dirs)
            for g in range(4 * dirs // SUB):
                for j in range(per):
                    seg_n[pl.ds(g * SUB * per + j, SUB, stride=per), :] = out[
                        g * SUB : (g + 1) * SUB, j * LANES : (j + 1) * LANES
                    ]

        def step_last(c):
            hops[c].wait_recv()
            lane = chunk_of(c)
            res[other, :, :, lane] = vis[other, :, :, lane] - got_c[turn, c]
            r = [[res[v // 4, v % 4, h * SUB : (h + 1) * SUB, lane] for h in range(halves)] for v in range(8)]
            for k in range(dirs):
                co = [[coh[k, v, h * SUB : (h + 1) * SUB, lane] for h in range(halves)] for v in range(8)]
                for a in range(4):
                    for b in range(4):
                        real = sum(r[a][h] * co[b][h] + r[4 + a][h] * co[4 + b][h] for h in range(halves))
                        imag = sum(r[4 + a][h] * co[b][h] - r[a][h] * co[4 + b][h] for h in range(halves))
                        n = 2 * (4 * a + b)
                        cross[n * dirs + k : n * dirs + k + 1, lane] = jnp.sum(real, axis=0, keepdims=True)
                        cross[(n + 1) * dirs + k : (n + 1) * dirs + k + 1, lane] = jnp.sum(
                            imag, axis=0, keepdims=True
                        )

            def crossed(a, b):
                n = 2 * (4 * a + b)
                return (
                    cross[n * dirs : (n + 1) * dirs, lane],
                    cross[(n + 1) * dirs : (n + 2) * dirs, lane],
                )

            jp, jq = ends_of(first_of(c)), ends_of(second_of(c))
            for which, j, other_end in ((0, jq, jp), (1, jp, jq)):
                where = second_of(c) if which else first_of(c)
                h00, h11, re01, im01 = [vals_n[n * dirs : (n + 1) * dirs, where] for n in range(4)]
                h01 = (re01, im01)
                for a in range(2):
                    for d in range(2):
                        total = None
                        for b in range(2):
                            for e in range(2):
                                if which == 0:
                                    term = cmul(j[2 * b + e], crossed(2 * a + b, 2 * d + e))
                                else:
                                    term = cmul_conj(j[2 * b + e], crossed(2 * b + a, 2 * e + d))
                                total = term if total is None else cadd(total, term)
                        if d == 0:
                            extra = cadd(scale(h00, other_end[2 * a]), cmul_conj(other_end[2 * a + 1], h01))
                        else:
                            extra = cadd(cmul(other_end[2 * a], h01), scale(h11, other_end[2 * a + 1]))
                        total = cadd(total, extra)
                        for part in range(2):
                            n = 4 * part + 2 * a + d
                            vals[n * dirs : (n + 1) * dirs, which * LANES : (which + 1) * LANES] = total[part]

            split_store(lhs_c, nrow, vals[...])
            rows = slice(2 * c * LANES, (2 * c + 2) * LANES)
            out = join(jnp.dot(lhs_c[...], scatter_hot[rows, :], preferred_element_type=f32), nrow)
            if c > 0:
                out = out + found[...]
            if c + 1 < chunks:
                found[...] = out
            else:
                for g in range(nrow // SUB):
                    for j in range(per):
                        seg[pl.ds(g * SUB * per + j, SUB, stride=per), :] = out[
                            g * SUB : (g + 1) * SUB, j * LANES : (j + 1) * LANES
                        ]

        if turn == 0:
            lax.fori_loop(0, chunks, gram_body, 0)
        for c in range(chunks):
            step_first(c)
        for c in range(chunks):
            normals(c)
        if turn == 0:
            scatter_setup()
        scatter_normals()
        if turn == 0:
            start_consensus()
            solve_weights()
            loads["vis"].wait()
        for stage in range(1, stages):
            for c in range(chunks):
                if stage + 1 == stages and c >= 2:
                    step_last(c - 2)
                step_next(stage, c)
                if turn > 0 and exchange and stage == 1 and c == ANSWER:
                    answer_parts(turn - 1)
        for c in range(max(0, chunks - 2) if stages > 1 else 0, chunks):
            step_last(c)

        def refresh(k, v, total, previous):
            here = packed(k, v)
            fresh = dual[here, :] + RHO * (jones[here, :] - total)
            if previous + 1 < ITERS:
                cons[here, :] = total
                dual[here, :] = fresh
            else:
                dual_out[halves_of(k, v)] = fresh

        def join_parts(previous):
            drain(consin.at[previous, pl.ds(1, n_band - 1)], p_recv.at[previous, 1])
            consin[previous, me] = outbox[previous, 0]
            for k in range(dirs):
                for v in range(8):
                    part, rows = part_of(k, v)
                    refresh(k, v, consin[previous, part, rows, :], previous)

        def ring_sum(turn, k, v, slots, total=None):
            for s in slots:
                term = weights[source(s)] * xall[ring(turn), k, s, v]
                total = term if total is None else total + term
            return total

        if turn > 0:
            if exchange:
                join_parts(turn - 1)
            else:
                for s in range(1, ahead + 1):
                    pump(turn - 1, s)
                for k in range(dirs):
                    for v in range(8):
                        refresh(k, v, ring_sum(turn - 1, k, v, range(n_band)), turn - 1)

        by_ring = turn + 1 == ITERS or not exchange
        for k in range(dirs):
            y = []
            for v in range(8):
                here = packed(k, v)
                y.append(seg[here, :] + RHO * cons[here, :] - dual[here, :])
            h00, h11, re01, im01 = [seg_n[packed(k, n), :] for n in range(4)]
            h00 = h00 + RHO
            h11 = h11 + RHO
            inverse = 1.0 / (h00 * h11 - (re01 * re01 + im01 * im01))
            h00, h11, h01 = h00 * inverse, h11 * inverse, (re01 * inverse, im01 * inverse)
            for a in range(2):
                y0, y1 = (y[2 * a], y[4 + 2 * a]), (y[2 * a + 1], y[4 + 2 * a + 1])
                minus0, minus1 = cmul_conj(y1, h01), cmul(y0, h01)
                for part in range(2):
                    for c in range(2):
                        if c == 0:
                            value = h11 * y0[part] - minus0[part]
                        else:
                            value = h00 * y1[part] - minus1[part]
                        v = 4 * part + 2 * a + c
                        here = packed(k, v)
                        jones[here, :] = value
                        if turn + 1 == ITERS:
                            jones_out[halves_of(k, v)] = value
                        sent = value + dual[here, :] * (1.0 / RHO)
                        if by_ring:
                            xall[ring(turn), k, 0, v] = sent
                        else:
                            chunk, rows = part_of(k, v)
                            xs[turn, chunk, rows, :] = sent
            if by_ring:
                for way in range(2):
                    if reach_of(k, way):
                        send_x(turn, k, way, 0)
        if not by_ring:
            send_parts(turn)

    last = ITERS - 1
    for s in range(1, ahead):
        pump(last, s)

    def coeff_body(slots, first):
        def run(m, carry):
            for k in range(dirs):
                total = [None] * 8 if first else [coeffs[(m,) + halves_of(k, v)] for v in range(8)]
                for s in slots:
                    factor = jnp.broadcast_to(gweights[source(s), pl.ds(m, 1), :], (SUB, LANES))
                    for v in range(8):
                        term = factor * xall[ring(last), k, s, v]
                        total[v] = term if total[v] is None else total[v] + term
                for v in range(8):
                    coeffs[(m,) + halves_of(k, v)] = total[v]
            return carry

        lax.fori_loop(0, SUB, run, 0)

    early = range(n_band - 1)
    coeff_body(early, True)
    for k in range(dirs):
        for v in range(8):
            cons[packed(k, v), :] = ring_sum(last, k, v, early)
    pump(last, ahead)
    late = range(n_band - 1, n_band)
    for k in range(dirs):
        for v in range(8):
            refresh(k, v, ring_sum(last, k, v, late, cons[packed(k, v), :]), last)
    coeff_body(late, False)

    drain(rows_all.at[pl.ds(1, n_band - 1)], row_send.at[0])
    drain(xall.at[:, :, pl.ds(1, n_band - 1)], x_send.at[0])
    if exchange:
        drain(inbox.at[:, pl.ds(1, n_band - 1)], p_send.at[0])
        drain(inbox.at[:, pl.ds(1, n_band - 1)], p_send.at[1])
    drain(got_a, d_send.at[0])
    for stage in range(1, stages):
        drain(got_a, d_send.at[stage])
    drain(got_a, d_send.at[stages])


def flush(*refs):
    count = (len(refs) - 1) // 2
    sem = refs[-1]
    copies = [pltpu.make_async_copy(refs[n], refs[count + n], sem.at[n]) for n in range(count)]
    for copy in copies:
        copy.start()
    for copy in copies:
        copy.wait()


def power_of_two(n):
    return n & (n - 1) == 0


def by_chunks(n_band, rows):
    return power_of_two(n_band) and rows % (n_band * SUB) == 0


def local(n_band, n_dir, vis, coh, jones_start, dual_start, consensus_start, freq_basis, pairs):
    f32 = jnp.float32
    dirs, times, base = coh.shape[1], coh.shape[-2], coh.shape[-1]
    stations = jones_start.shape[-1]
    per = stations // LANES
    nrow = 8 * dirs
    terms = freq_basis.shape[1]

    def enter(value):
        lead = value.shape[:-2]
        value = value.reshape(lead + (2, per, LANES))
        return jnp.swapaxes(value, -2, -3).reshape(lead + (2 * per, LANES))

    def leave(value, shape):
        value = value.reshape(value.shape[:-2] + (per, 2, LANES))
        return jnp.swapaxes(value, -2, -3).reshape(shape)

    stages = n_dir.bit_length() - 1
    chunks = base // LANES
    exchange = by_chunks(n_band, nrow * per)
    rings = 1 if exchange else ITERS
    parts = (ITERS - 1, n_band, max(SUB, nrow * per // n_band), LANES) if exchange else (1, 1, SUB, LANES)
    half = (4, times, base)
    piece = (4, times, LANES)
    vmem = pl.BlockSpec(memory_space=pltpu.VMEM)
    far = pl.BlockSpec(memory_space=pltpu.HBM)
    raw = (dirs, 4, 2 * per, LANES)
    raw_out = jax.ShapeDtypeStruct(raw, f32)
    raw_terms = jax.ShapeDtypeStruct((terms,) + raw, f32)
    bf16 = jnp.bfloat16
    operands = (
        vis.reshape((2,) + half),
        coh.reshape(dirs, 8, times, base),
        enter(jones_start.reshape((dirs, 4, 2, stations))),
        enter(dual_start.reshape((dirs, 4, 2, stations))),
        enter(consensus_start.reshape((terms, dirs, 4, 2, stations))),
        freq_basis,
        pairs,
    )
    results = pl.pallas_call(
        functools.partial(kernel, n_band, n_dir, dirs, times, base, stations),
        out_shape=(pltpu.VMEM(raw, f32), pltpu.VMEM(raw, f32), pltpu.VMEM((terms,) + raw, f32)),
        in_specs=[far] * 7,
        out_specs=(vmem,) * 3,
        scratch_shapes=[
            pltpu.VMEM((2,) + half, f32),
            pltpu.VMEM((dirs, 8, times, base), f32),
            pltpu.VMEM(raw, f32),
            pltpu.VMEM(raw, f32),
            pltpu.VMEM((terms,) + raw, f32),
            pltpu.SMEM(freq_basis.shape, f32),
            pltpu.VMEM((2, base), jnp.int32),
            pltpu.VMEM((nrow * per, LANES), f32),
            pltpu.VMEM((nrow * per, LANES), f32),
            pltpu.VMEM((SUB, LANES), f32),
            pltpu.VMEM((2 * base, LANES), jnp.int32),
            pltpu.VMEM((nrow * per, LANES), f32),
            pltpu.VMEM((rings, dirs, n_band, 8, per, LANES), f32),
            pltpu.VMEM((n_band, SUB, LANES), f32),
            pltpu.VMEM((n_band, SUB, LANES), f32),
            pltpu.VMEM((n_band, SUB, LANES), f32),
            pltpu.VMEM((n_band * n_band if exchange else 1, SUB, LANES), f32),
            pltpu.VMEM(parts, f32),
            pltpu.VMEM(parts, f32),
            pltpu.VMEM(parts, f32),
            pltpu.VMEM(parts, f32),
            pltpu.VMEM((stations, 2 * base), bf16),
            pltpu.VMEM((2 * base, stations), bf16),
            pltpu.VMEM((PIECES * nrow, stations), bf16),
            pltpu.VMEM((PIECES * nrow, 2 * LANES), bf16),
            pltpu.VMEM((PIECES * 4 * dirs, 2 * base), bf16),
            pltpu.VMEM((nrow, 2 * base), f32),
            pltpu.VMEM((20 * dirs, base), f32),
            pltpu.VMEM((32 * dirs, base), f32),
            pltpu.VMEM((nrow, 2 * LANES), f32),
            pltpu.VMEM((4 * dirs, 2 * base), f32),
            pltpu.VMEM((nrow, stations), f32),
            pltpu.VMEM((nrow * per, LANES), f32),
            pltpu.VMEM((4 * dirs * per, LANES), f32),
            pltpu.VMEM((ITERS, chunks, 2) + piece, f32),
            pltpu.VMEM((ITERS, chunks) + piece, f32),
            pltpu.VMEM((ITERS, stages, chunks) + piece, f32),
            pltpu.VMEM((ITERS, max(1, stages - 1), chunks) + piece, f32),
            pltpu.VMEM((ITERS, chunks) + piece, f32),
            pltpu.VMEM((2,) + half, f32),
            pltpu.SemaphoreType.DMA((7,)),
            pltpu.SemaphoreType.DMA((1,)),
            pltpu.SemaphoreType.DMA((1,)),
            pltpu.SemaphoreType.DMA((2,)),
            pltpu.SemaphoreType.DMA((ITERS - 1, 2)),
            pltpu.SemaphoreType.DMA((1,)),
            pltpu.SemaphoreType.DMA((rings, dirs, n_band - 1)),
            pltpu.SemaphoreType.DMA((stages + 1,)),
            pltpu.SemaphoreType.DMA((ITERS, stages + 1, chunks)),
        ],
        compiler_params=pltpu.CompilerParams(
            collective_id=0, has_side_effects=True, vmem_limit_bytes=56 * 1024 * 1024
        ),
    )(*[pltpu.with_memory_space_constraint(x, pltpu.HBM) for x in operands])
    jones, dual, coeffs = pl.pallas_call(
        flush,
        out_shape=(raw_out, raw_out, raw_terms),
        in_specs=[vmem] * 3,
        out_specs=(pl.BlockSpec(memory_space=pltpu.HBM),) * 3,
        scratch_shapes=[pltpu.SemaphoreType.DMA((3,))],
        compiler_params=pltpu.CompilerParams(vmem_limit_bytes=1024 * 1024),
    )(*[pltpu.with_memory_space_constraint(x, pltpu.VMEM) for x in results])
    return (
        leave(jones, jones_start.shape),
        leave(dual, jones_start.shape),
        leave(coeffs, consensus_start.shape),
    )


def solution(mesh):
    in_specs = (
        P("band", None, None, None, None, None),
        P("band", "dir", None, None, None, None, None),
        P("band", "dir", None, None, None, None),
        P("band", "dir", None, None, None, None),
        P(None, "dir", None, None, None, None),
        P("band", None),
        P(),
    )
    out_specs = (
        P("band", "dir", None, None, None, None),
        P("band", "dir", None, None, None, None),
        P(None, "dir", None, None, None, None),
    )
    body = functools.partial(local, mesh.shape["band"], mesh.shape["dir"])
    return jax.shard_map(body, mesh=mesh, in_specs=in_specs, out_specs=out_specs, check_vma=False)
```

```python
import functools

import jax
import jax.numpy as jnp
from jax import lax
from jax.experimental import pallas as pl
from jax.experimental.pallas import tpu as pltpu
from jax.sharding import PartitionSpec as P

ITERS = 3
RHO = 5.0
RIDGE = 0.25
LANES = 128
SUB = 8
PIECES = 3
ANSWER = 0
MESH = pl.DeviceIdType.MESH


def cmul(a, b):
    return (a[0] * b[0] - a[1] * b[1], a[0] * b[1] + a[1] * b[0])


def cmul_conj(a, b):
    return (a[0] * b[0] + a[1] * b[1], a[1] * b[0] - a[0] * b[1])


def cadd(a, b):
    return (a[0] + b[0], a[1] + b[1])


def conj(a):
    return (a[0], -a[1])


def re_mul(a, b):
    return a[0] * b[0] - a[1] * b[1]


def scale(r, a):
    return (r * a[0], r * a[1])


def split_store(ref, rows, value):
    left = value
    for piece in range(PIECES):
        part = left.astype(jnp.bfloat16)
        ref[piece * rows : (piece + 1) * rows, :] = part
        if piece + 1 < PIECES:
            left = left - part.astype(jnp.float32)


def join(value, rows):
    total = value[0:rows]
    for piece in range(1, PIECES):
        total = total + value[piece * rows : (piece + 1) * rows]
    return total


def kernel(
    n_band, n_dir, dirs, times, base, stations,
    vis_far, coh_far, jones0_far, dual0_far, coeffs0_far, basis_far, pairs_far,
    jones_out, dual_out, coeffs,
    vis, coh, jones0, dual0, coeffs0, basis, pairs_ref,
    jones, dual, row, ids_col,
    cons, xall, rows_all, weights, gweights, wmat,
    xs, inbox, outbox, consin,
    gather_hot, scatter_hot, lhs, lhs_c, lhs_n, ends, grams, cross, vals, vals_n, found, seg, seg_n,
    model, got_a, sums, got_b, got_c, res,
    load_sem, row_send, row_recv, p_send, p_recv, x_send, x_recv, d_send, d_recv,
):
    f32 = jnp.float32
    nrow = 8 * dirs
    per = stations // LANES
    me = lax.axis_index("band")
    mine = lax.axis_index("dir")
    chunks = base // LANES
    halves = times // SUB
    stages = n_dir.bit_length() - 1
    part_rows = nrow * per // n_band
    exchange = by_chunks(n_band, nrow * per)

    def at(pos):
        half = pos // (n_band // 2)
        return (1 - half) * (2 * pos) + half * (2 * (n_band - 1 - pos) + 1)

    odd = lax.rem(me, 2)
    pos = (1 - odd) * (me // 2) + odd * (n_band - 1 - me // 2)
    nexts = (at(lax.rem(pos + 1, n_band)), at(lax.rem(pos + n_band - 1, n_band)))

    def flip_bits(index, mask):
        out = index
        for b in range(mask.bit_length()):
            if mask >> b & 1:
                out = out + (1 - 2 * lax.rem(index // (1 << b), 2)) * (1 << b)
        return out

    def to_of(step):
        return flip_bits(me, step) if power_of_two(n_band) else lax.rem(me + step, n_band)

    def from_of(step):
        return flip_bits(me, step) if power_of_two(n_band) else lax.rem(me + n_band - step, n_band)

    def flip(stage):
        return flip_bits(mine, 1 << stage)

    def drain(ref, sem):
        pltpu.make_async_copy(ref, ref, sem).wait()

    own = lax.rem(mine, 2)
    other = 1 - own

    loads = {}
    for n, (name, source_ref, near) in enumerate((
        ("pairs", pairs_far, pairs_ref),
        ("jones", jones0_far, jones0),
        ("coh", coh_far, coh),
        ("basis", basis_far, basis),
        ("vis", vis_far, vis),
        ("dual", dual0_far, dual0),
        ("coeffs", coeffs0_far, coeffs0),
    )):
        loads[name] = pltpu.make_async_copy(source_ref, near, load_sem.at[n])
        loads[name].start()

    barrier = pltpu.get_barrier_semaphore()
    for step in range(1, n_band):
        pl.semaphore_signal(barrier, inc=1, device_id={"band": to_of(step)}, device_id_type=MESH)
    for stage in range(stages):
        pl.semaphore_signal(barrier, inc=1, device_id={"dir": flip(stage)}, device_id_type=MESH)

    def halves_of(k, v):
        return (k, v // 2, pl.ds(v % 2, per, stride=2), slice(None))

    def packed(k, v):
        return pl.ds((v * dirs + k) * per, per)

    def block_of(j):
        return j % 2, (j // 2) * LANES

    step_rows = 32

    def hot_body(i, carry):
        start = pl.multiple_of(i * step_rows, step_rows)
        for j in range(2 * chunks):
            lane = slice(j * LANES, (j + 1) * LANES)
            sid = lax.broadcasted_iota(jnp.int32, (step_rows, LANES), 0) + i * step_rows
            which, low = block_of(j)
            ids = pairs_ref[which : which + 1, low : low + LANES]
            same = sid == jnp.broadcast_to(ids, (step_rows, LANES))
            gather_hot[pl.ds(start, step_rows), lane] = jnp.where(same, 1.0, 0.0).astype(jnp.bfloat16)
        return carry

    loads["pairs"].wait()
    lax.fori_loop(0, stations // step_rows, hot_body, 0)

    loads["jones"].wait()
    for k in range(dirs):
        for v in range(8):
            jones[packed(k, v), :] = jones0[halves_of(k, v)]

    def scatter_setup():
        for j in range(2 * chunks):
            which, low = block_of(j)
            ids = jnp.broadcast_to(pairs_ref[which : which + 1, low : low + LANES], (LANES, LANES))
            ids_col[j * LANES : (j + 1) * LANES, :] = jnp.transpose(ids)

        def hot_body2(i, carry):
            start = pl.multiple_of(i * step_rows, step_rows)
            col = ids_col[pl.ds(start, step_rows), :]
            for j in range(stations // LANES):
                lane = slice(j * LANES, (j + 1) * LANES)
                sid = lax.broadcasted_iota(jnp.int32, (step_rows, LANES), 1) + j * LANES
                scatter_hot[pl.ds(start, step_rows), lane] = jnp.where(sid == col, 1.0, 0.0).astype(jnp.bfloat16)
            return carry

        lax.fori_loop(0, 2 * base // step_rows, hot_body2, 0)

    def first_sends():
        pl.semaphore_wait(barrier, n_band - 1 + stages)
        loads["basis"].wait()
        row[...] = jnp.zeros((SUB, LANES), f32)
        for m in range(SUB):
            row[m : m + 1, :] = jnp.full((1, LANES), basis[0, m], f32)
        for step in range(1, n_band):
            pltpu.make_async_remote_copy(
                src_ref=row,
                dst_ref=rows_all.at[step],
                send_sem=row_send.at[0],
                recv_sem=row_recv.at[0],
                device_id={"band": to_of(step)},
                device_id_type=MESH,
            ).start()

    pairs = [(a, b) for a in range(4) for b in range(a, 4)]

    def gram_body(j, carry):
        lane = pl.ds(pl.multiple_of(j * LANES, LANES), LANES)
        for k in range(dirs):
            c = [
                [coh[k, v, h * SUB : (h + 1) * SUB, lane] for h in range(halves)]
                for v in range(8)
            ]
            for n, (a, b) in enumerate(pairs):
                real = sum(c[a][h] * c[b][h] + c[4 + a][h] * c[4 + b][h] for h in range(halves))
                grams[(2 * n) * dirs + k : (2 * n) * dirs + k + 1, lane] = jnp.sum(real, axis=0, keepdims=True)
                if a != b:
                    imag = sum(c[4 + a][h] * c[b][h] - c[a][h] * c[4 + b][h] for h in range(halves))
                    grams[(2 * n + 1) * dirs + k : (2 * n + 1) * dirs + k + 1, lane] = jnp.sum(
                        imag, axis=0, keepdims=True
                    )
        return carry

    def start_consensus():
        loads["coeffs"].wait()
        loads["dual"].wait()
        for k in range(dirs):
            for v in range(8):
                dual[packed(k, v), :] = dual0[halves_of(k, v)]
                total = basis[0, 0] * coeffs0[(0,) + halves_of(k, v)]
                for m in range(1, SUB):
                    total = total + basis[0, m] * coeffs0[(m,) + halves_of(k, v)]
                cons[packed(k, v), :] = total

    def solve_weights():
        drain(rows_all.at[pl.ds(1, n_band - 1)], row_recv.at[0])
        rows_all[0] = row[...]
        held = [rows_all[s] for s in range(n_band)]
        columns = []
        for m in range(SUB):
            total = held[0] * held[0][m : m + 1, :]
            for s in range(1, n_band):
                total = total + held[s] * held[s][m : m + 1, :]
            ident = jnp.where(lax.broadcasted_iota(jnp.int32, (SUB, LANES), 0) == m, RIDGE * n_band, 0.0)
            columns.append(total + ident.astype(f32))
        right = list(held)
        iota = lax.broadcasted_iota(jnp.int32, (SUB, LANES), 0)
        for i in range(SUB):
            inverse = 1.0 / columns[i][i : i + 1, :]
            factor = columns[i]
            for group in (columns, right):
                for c in range(len(group)):
                    lead = jnp.broadcast_to(group[c][i : i + 1, :] * inverse, (SUB, LANES))
                    group[c] = jnp.where(iota == i, lead, group[c] - factor * lead)

        def weight_of(a, b):
            return jnp.broadcast_to(jnp.sum(right[b] * held[a], axis=0, keepdims=True), (SUB, LANES))

        for s in range(n_band):
            band = from_of(s)
            gweights[band] = right[s]
            weights[band] = weight_of(0, s)
        if exchange:
            for a in range(n_band):
                for b in range(n_band):
                    wmat[a * n_band + b] = weight_of(a, b)

    x_copies = [{} for _ in range(ITERS)]
    ahead = n_band // 2
    behind = n_band - 1 - ahead

    def ring(turn):
        return 0 if exchange else turn

    def slot_of(way, distance):
        if distance > behind:
            return n_band - 1
        return distance + way * behind if distance else 0

    cuts = ring_cuts(exchange)
    units = dirs * cuts

    def reach_of(u, way):
        return ahead if way == u % 2 else behind

    order = [
        (u, way)
        for pair in zip(*[sorted(range(units), key=lambda u: -reach_of(u, way)) for way in range(2)])
        for way, u in enumerate(pair)
    ]

    def send_x(turn, u, way, distance):
        to = slot_of(way, distance + 1)
        k, rows = u // cuts, pl.ds(u % cuts * (8 // cuts), 8 // cuts)
        copy = pltpu.make_async_remote_copy(
            src_ref=xall.at[ring(turn), k, slot_of(way, distance), rows],
            dst_ref=xall.at[ring(turn), k, to, rows],
            send_sem=x_send.at[0],
            recv_sem=x_recv.at[ring(turn), u, to - 1],
            device_id={"band": nexts[way]},
            device_id_type=MESH,
        )
        copy.start()
        x_copies[turn][(u, way, distance + 1)] = copy

    def pump(turn, distance):
        for u, way in order:
            reach = reach_of(u, way)
            if distance <= reach:
                x_copies[turn][(u, way, distance)].wait_recv()
                if distance < reach:
                    send_x(turn, u, way, distance)

    def source(slot):
        if slot <= behind:
            return at(lax.rem(pos + n_band - slot, n_band))
        return at(lax.rem(pos + slot - behind, n_band))

    def part_of(k, v):
        here = (v * dirs + k) * per
        return here // part_rows, pl.ds(here % part_rows, per)

    def send_parts(turn):
        for step in range(n_band - 1, 0, -1):
            pltpu.make_async_remote_copy(
                src_ref=xs.at[turn, to_of(step)],
                dst_ref=inbox.at[turn, step],
                send_sem=p_send.at[0],
                recv_sem=p_recv.at[turn, 0],
                device_id={"band": to_of(step)},
                device_id_type=MESH,
            ).start()

    def answer_parts(turn):
        drain(inbox.at[turn, pl.ds(1, n_band - 1)], p_recv.at[turn, 0])
        inbox[turn, 0] = xs[turn, me]
        for a in range(n_band - 1, -1, -1):
            for r in range(part_rows // SUB):
                here = slice(r * SUB, (r + 1) * SUB)
                total = wmat[a * n_band] * inbox[turn, 0, here, :]
                for b in range(1, n_band):
                    total = total + wmat[a * n_band + b] * inbox[turn, b, here, :]
                outbox[turn, a, here, :] = total
            if a:
                pltpu.make_async_remote_copy(
                    src_ref=outbox.at[turn, a],
                    dst_ref=consin.at[turn, me],
                    send_sem=p_send.at[1],
                    recv_sem=p_recv.at[turn, 1],
                    device_id={"band": to_of(a)},
                    device_id_type=MESH,
                ).start()

    def send_d(turn, n, c, src, dst, stage):
        copy = pltpu.make_async_remote_copy(
            src_ref=src,
            dst_ref=dst,
            send_sem=d_send.at[n],
            recv_sem=d_recv.at[turn, n, c],
            device_id={"dir": flip(stage)},
            device_id_type=MESH,
        )
        copy.start()
        return copy

    def end(comp, lane):
        return ends[comp * dirs : (comp + 1) * dirs, lane]

    def gram(a, b, lane):
        if a > b:
            return conj(gram(b, a, lane))
        n = pairs.index((a, b))
        real = grams[(2 * n) * dirs : (2 * n + 1) * dirs, lane]
        if a == b:
            return real
        return (real, grams[(2 * n + 1) * dirs : (2 * n + 2) * dirs, lane])

    def first_of(c):
        return slice(2 * c * LANES, (2 * c + 1) * LANES)

    def second_of(c):
        return slice((2 * c + 1) * LANES, (2 * c + 2) * LANES)

    def chunk_of(c):
        return slice(c * LANES, (c + 1) * LANES)

    for turn in range(ITERS):
        for g in range(nrow // SUB):
            for j in range(per):
                left = jones[pl.ds(g * SUB * per + j, SUB, stride=per), :]
                for piece in range(PIECES):
                    part = left.astype(jnp.bfloat16)
                    lhs[
                        piece * nrow + g * SUB : piece * nrow + (g + 1) * SUB,
                        j * LANES : (j + 1) * LANES,
                    ] = part
                    left = left - part.astype(f32)
        ends[...] = join(jnp.dot(lhs[...], gather_hot[...], preferred_element_type=f32), nrow)

        def predict(c):
            lane, lane_p, lane_q = chunk_of(c), first_of(c), second_of(c)

            def model_body(h, carry):
                time = pl.ds(pl.multiple_of(h * SUB, SUB), SUB)
                total = [None] * 4
                for k in range(dirs):
                    co = [(coh[k, v, time, lane], coh[k, 4 + v, time, lane]) for v in range(4)]

                    def spread(v, where):
                        return tuple(
                            jnp.broadcast_to(
                                ends[(4 * part + v) * dirs + k : (4 * part + v) * dirs + k + 1, where],
                                (SUB, LANES),
                            )
                            for part in range(2)
                        )

                    p = [spread(v, lane_p) for v in range(4)]
                    q = [spread(v, lane_q) for v in range(4)]
                    for a in range(2):
                        b = [cadd(cmul(p[2 * a], co[d]), cmul(p[2 * a + 1], co[2 + d])) for d in range(2)]
                        for d in range(2):
                            term = cadd(cmul_conj(b[0], q[2 * d]), cmul_conj(b[1], q[2 * d + 1]))
                            v = 2 * a + d
                            total[v] = term if total[v] is None else cadd(total[v], term)
                for v in range(4):
                    model[turn, c, 0, v, time, :] = total[v][0]
                    model[turn, c, 1, v, time, :] = total[v][1]
                return carry

            lax.fori_loop(0, halves, model_body, 0)

        if turn == 0:
            loads["coh"].wait()
        hops = []
        for c in range(chunks):
            predict(c)
            if turn == 0 and c == 0:
                first_sends()
            hops.append(send_d(turn, 0, c, model.at[turn, c, other], got_a.at[turn, c], 0))

        def step_first(c):
            hops[c].wait_recv()
            sums[turn, 0, c] = model[turn, c, own] + got_a[turn, c]
            n = 1
            if stages > 1:
                hops[c] = send_d(turn, n, c, sums.at[turn, 0, c], got_b.at[turn, 0, c], 1)
            else:
                share(c)

        def share(c):
            hops[c] = send_d(turn, stages, c, sums.at[turn, stages - 1, c], got_c.at[turn, c], 0)
            lane = chunk_of(c)
            res[own, :, :, lane] = vis[own, :, :, lane] - sums[turn, stages - 1, c]

        def step_next(stage, c):
            hops[c].wait_recv()
            sums[turn, stage, c] = sums[turn, stage - 1, c] + got_b[turn, stage - 1, c]
            if stage + 1 < stages:
                hops[c] = send_d(
                    turn, stage + 1, c, sums.at[turn, stage, c], got_b.at[turn, stage, c], stage + 1
                )
            else:
                share(c)

        def gram_of(j):
            m00 = re_mul(j[0], conj(j[0])) + re_mul(j[2], conj(j[2]))
            m11 = re_mul(j[1], conj(j[1])) + re_mul(j[3], conj(j[3]))
            m01 = cadd(cmul_conj(j[1], j[0]), cmul_conj(j[3], j[2]))
            return m00, m11, m01

        def ends_of(lane):
            return [(end(v, lane), end(4 + v, lane)) for v in range(4)]

        def normals(c):
            lane = chunk_of(c)

            def gr(a, b):
                return gram(a, b, lane)

            jp, jq = ends_of(first_of(c)), ends_of(second_of(c))
            m00, m11, m01 = gram_of(jq)
            p00, p11, p01 = gram_of(jp)
            n1_00 = m00 * gr(0, 0) + m11 * gr(1, 1) + 2.0 * re_mul(m01, gr(0, 1))
            n1_11 = m00 * gr(2, 2) + m11 * gr(3, 3) + 2.0 * re_mul(m01, gr(2, 3))
            n1_01 = cadd(
                cadd(scale(m00, gr(0, 2)), scale(m11, gr(1, 3))),
                cadd(cmul(m01, gr(0, 3)), cmul(conj(m01), gr(1, 2))),
            )
            n2_00 = p00 * gr(0, 0) + p11 * gr(2, 2) + 2.0 * re_mul(p01, gr(2, 0))
            n2_11 = p00 * gr(1, 1) + p11 * gr(3, 3) + 2.0 * re_mul(p01, gr(3, 1))
            n2_01 = cadd(
                cadd(scale(p00, gr(1, 0)), scale(p11, gr(3, 2))),
                cadd(cmul(p01, gr(3, 0)), cmul(conj(p01), gr(1, 2))),
            )
            for n, (left, right) in enumerate(
                ((n1_00, n2_00), (n1_11, n2_11), (n1_01[0], n2_01[0]), (n1_01[1], n2_01[1]))
            ):
                vals_n[n * dirs : (n + 1) * dirs, first_of(c)] = left
                vals_n[n * dirs : (n + 1) * dirs, second_of(c)] = right

        def scatter_normals():
            split_store(lhs_n, 4 * dirs, vals_n[...])
            out = join(jnp.dot(lhs_n[...], scatter_hot[...], preferred_element_type=f32), 4 * dirs)
            for g in range(4 * dirs // SUB):
                for j in range(per):
                    seg_n[pl.ds(g * SUB * per + j, SUB, stride=per), :] = out[
                        g * SUB : (g + 1) * SUB, j * LANES : (j + 1) * LANES
                    ]

        def step_last(c):
            hops[c].wait_recv()
            lane = chunk_of(c)
            res[other, :, :, lane] = vis[other, :, :, lane] - got_c[turn, c]
            r = [[res[v // 4, v % 4, h * SUB : (h + 1) * SUB, lane] for h in range(halves)] for v in range(8)]
            for k in range(dirs):
                co = [[coh[k, v, h * SUB : (h + 1) * SUB, lane] for h in range(halves)] for v in range(8)]
                for a in range(4):
                    for b in range(4):
                        real = sum(r[a][h] * co[b][h] + r[4 + a][h] * co[4 + b][h] for h in range(halves))
                        imag = sum(r[4 + a][h] * co[b][h] - r[a][h] * co[4 + b][h] for h in range(halves))
                        n = 2 * (4 * a + b)
                        cross[n * dirs + k : n * dirs + k + 1, lane] = jnp.sum(real, axis=0, keepdims=True)
                        cross[(n + 1) * dirs + k : (n + 1) * dirs + k + 1, lane] = jnp.sum(
                            imag, axis=0, keepdims=True
                        )

            def crossed(a, b):
                n = 2 * (4 * a + b)
                return (
                    cross[n * dirs : (n + 1) * dirs, lane],
                    cross[(n + 1) * dirs : (n + 2) * dirs, lane],
                )

            jp, jq = ends_of(first_of(c)), ends_of(second_of(c))
            for which, j, other_end in ((0, jq, jp), (1, jp, jq)):
                where = second_of(c) if which else first_of(c)
                h00, h11, re01, im01 = [vals_n[n * dirs : (n + 1) * dirs, where] for n in range(4)]
                h01 = (re01, im01)
                for a in range(2):
                    for d in range(2):
                        total = None
                        for b in range(2):
                            for e in range(2):
                                if which == 0:
                                    term = cmul(j[2 * b + e], crossed(2 * a + b, 2 * d + e))
                                else:
                                    term = cmul_conj(j[2 * b + e], crossed(2 * b + a, 2 * e + d))
                                total = term if total is None else cadd(total, term)
                        if d == 0:
                            extra = cadd(scale(h00, other_end[2 * a]), cmul_conj(other_end[2 * a + 1], h01))
                        else:
                            extra = cadd(cmul(other_end[2 * a], h01), scale(h11, other_end[2 * a + 1]))
                        total = cadd(total, extra)
                        for part in range(2):
                            n = 4 * part + 2 * a + d
                            vals[n * dirs : (n + 1) * dirs, which * LANES : (which + 1) * LANES] = total[part]

            split_store(lhs_c, nrow, vals[...])
            rows = slice(2 * c * LANES, (2 * c + 2) * LANES)
            out = join(jnp.dot(lhs_c[...], scatter_hot[rows, :], preferred_element_type=f32), nrow)
            if c > 0:
                out = out + found[...]
            if c + 1 < chunks:
                found[...] = out
            else:
                for g in range(nrow // SUB):
                    for j in range(per):
                        seg[pl.ds(g * SUB * per + j, SUB, stride=per), :] = out[
                            g * SUB : (g + 1) * SUB, j * LANES : (j + 1) * LANES
                        ]

        if turn == 0:
            lax.fori_loop(0, chunks, gram_body, 0)
        for c in range(chunks):
            step_first(c)
        for c in range(chunks):
            normals(c)
        if turn == 0:
            scatter_setup()
        scatter_normals()
        if turn == 0:
            start_consensus()
            solve_weights()
            loads["vis"].wait()
        for stage in range(1, stages):
            for c in range(chunks):
                if stage + 1 == stages and c >= 2:
                    step_last(c - 2)
                step_next(stage, c)
                if turn > 0 and exchange and stage == 1 and c == ANSWER:
                    answer_parts(turn - 1)
        for c in range(max(0, chunks - 2) if stages > 1 else 0, chunks):
            step_last(c)

        def refresh(k, v, total, previous):
            here = packed(k, v)
            fresh = dual[here, :] + RHO * (jones[here, :] - total)
            if previous + 1 < ITERS:
                cons[here, :] = total
                dual[here, :] = fresh
            else:
                dual_out[halves_of(k, v)] = fresh

        def join_parts(previous):
            drain(consin.at[previous, pl.ds(1, n_band - 1)], p_recv.at[previous, 1])
            consin[previous, me] = outbox[previous, 0]
            for k in range(dirs):
                for v in range(8):
                    part, rows = part_of(k, v)
                    refresh(k, v, consin[previous, part, rows, :], previous)

        def ring_sum(turn, k, v, slots, total=None):
            for s in slots:
                term = weights[source(s)] * xall[ring(turn), k, s, v]
                total = term if total is None else total + term
            return total

        if turn > 0:
            if exchange:
                join_parts(turn - 1)
            else:
                for s in range(1, ahead + 1):
                    pump(turn - 1, s)
                for k in range(dirs):
                    for v in range(8):
                        refresh(k, v, ring_sum(turn - 1, k, v, range(n_band)), turn - 1)

        by_ring = turn + 1 == ITERS or not exchange
        for k in range(dirs):
            y = []
            for v in range(8):
                here = packed(k, v)
                y.append(seg[here, :] + RHO * cons[here, :] - dual[here, :])
            h00, h11, re01, im01 = [seg_n[packed(k, n), :] for n in range(4)]
            h00 = h00 + RHO
            h11 = h11 + RHO
            inverse = 1.0 / (h00 * h11 - (re01 * re01 + im01 * im01))
            h00, h11, h01 = h00 * inverse, h11 * inverse, (re01 * inverse, im01 * inverse)
            for a in range(2):
                y0, y1 = (y[2 * a], y[4 + 2 * a]), (y[2 * a + 1], y[4 + 2 * a + 1])
                minus0, minus1 = cmul_conj(y1, h01), cmul(y0, h01)
                for part in range(2):
                    for c in range(2):
                        if c == 0:
                            value = h11 * y0[part] - minus0[part]
                        else:
                            value = h00 * y1[part] - minus1[part]
                        v = 4 * part + 2 * a + c
                        here = packed(k, v)
                        jones[here, :] = value
                        if turn + 1 == ITERS:
                            jones_out[halves_of(k, v)] = value
                        sent = value + dual[here, :] * (1.0 / RHO)
                        if by_ring:
                            xall[ring(turn), k, 0, v] = sent
                        else:
                            chunk, rows = part_of(k, v)
                            xs[turn, chunk, rows, :] = sent
        if by_ring:
            for u, way in order:
                if reach_of(u, way):
                    send_x(turn, u, way, 0)
        else:
            send_parts(turn)

    last = ITERS - 1
    for s in range(1, ahead):
        pump(last, s)

    def coeff_body(slots, first):
        def run(m, carry):
            for k in range(dirs):
                total = [None] * 8 if first else [coeffs[(m,) + halves_of(k, v)] for v in range(8)]
                for s in slots:
                    factor = jnp.broadcast_to(gweights[source(s), pl.ds(m, 1), :], (SUB, LANES))
                    for v in range(8):
                        term = factor * xall[ring(last), k, s, v]
                        total[v] = term if total[v] is None else total[v] + term
                for v in range(8):
                    coeffs[(m,) + halves_of(k, v)] = total[v]
            return carry

        lax.fori_loop(0, SUB, run, 0)

    early = range(n_band - 1)
    coeff_body(early, True)
    for k in range(dirs):
        for v in range(8):
            cons[packed(k, v), :] = ring_sum(last, k, v, early)
    pump(last, ahead)
    late = range(n_band - 1, n_band)
    for k in range(dirs):
        for v in range(8):
            refresh(k, v, ring_sum(last, k, v, late, cons[packed(k, v), :]), last)
    coeff_body(late, False)

    drain(rows_all.at[pl.ds(1, n_band - 1)], row_send.at[0])
    drain(xall.at[:, :, pl.ds(1, n_band - 1)], x_send.at[0])
    if exchange:
        drain(inbox.at[:, pl.ds(1, n_band - 1)], p_send.at[0])
        drain(inbox.at[:, pl.ds(1, n_band - 1)], p_send.at[1])
    drain(got_a, d_send.at[0])
    for stage in range(1, stages):
        drain(got_a, d_send.at[stage])
    drain(got_a, d_send.at[stages])


def flush(*refs):
    count = (len(refs) - 1) // 2
    sem = refs[-1]
    copies = [pltpu.make_async_copy(refs[n], refs[count + n], sem.at[n]) for n in range(count)]
    for copy in copies:
        copy.start()
    for copy in copies:
        copy.wait()


def power_of_two(n):
    return n & (n - 1) == 0


def ring_cuts(exchange):
    return 2 if exchange else 1


def by_chunks(n_band, rows):
    return power_of_two(n_band) and rows % (n_band * SUB) == 0


def local(n_band, n_dir, vis, coh, jones_start, dual_start, consensus_start, freq_basis, pairs):
    f32 = jnp.float32
    dirs, times, base = coh.shape[1], coh.shape[-2], coh.shape[-1]
    stations = jones_start.shape[-1]
    per = stations // LANES
    nrow = 8 * dirs
    terms = freq_basis.shape[1]

    def enter(value):
        lead = value.shape[:-2]
        value = value.reshape(lead + (2, per, LANES))
        return jnp.swapaxes(value, -2, -3).reshape(lead + (2 * per, LANES))

    def leave(value, shape):
        value = value.reshape(value.shape[:-2] + (per, 2, LANES))
        return jnp.swapaxes(value, -2, -3).reshape(shape)

    stages = n_dir.bit_length() - 1
    chunks = base // LANES
    exchange = by_chunks(n_band, nrow * per)
    rings = 1 if exchange else ITERS
    parts = (ITERS - 1, n_band, max(SUB, nrow * per // n_band), LANES) if exchange else (1, 1, SUB, LANES)
    half = (4, times, base)
    piece = (4, times, LANES)
    vmem = pl.BlockSpec(memory_space=pltpu.VMEM)
    far = pl.BlockSpec(memory_space=pltpu.HBM)
    raw = (dirs, 4, 2 * per, LANES)
    raw_out = jax.ShapeDtypeStruct(raw, f32)
    raw_terms = jax.ShapeDtypeStruct((terms,) + raw, f32)
    bf16 = jnp.bfloat16
    operands = (
        vis.reshape((2,) + half),
        coh.reshape(dirs, 8, times, base),
        enter(jones_start.reshape((dirs, 4, 2, stations))),
        enter(dual_start.reshape((dirs, 4, 2, stations))),
        enter(consensus_start.reshape((terms, dirs, 4, 2, stations))),
        freq_basis,
        pairs,
    )
    results = pl.pallas_call(
        functools.partial(kernel, n_band, n_dir, dirs, times, base, stations),
        out_shape=(pltpu.VMEM(raw, f32), pltpu.VMEM(raw, f32), pltpu.VMEM((terms,) + raw, f32)),
        in_specs=[far] * 7,
        out_specs=(vmem,) * 3,
        scratch_shapes=[
            pltpu.VMEM((2,) + half, f32),
            pltpu.VMEM((dirs, 8, times, base), f32),
            pltpu.VMEM(raw, f32),
            pltpu.VMEM(raw, f32),
            pltpu.VMEM((terms,) + raw, f32),
            pltpu.SMEM(freq_basis.shape, f32),
            pltpu.VMEM((2, base), jnp.int32),
            pltpu.VMEM((nrow * per, LANES), f32),
            pltpu.VMEM((nrow * per, LANES), f32),
            pltpu.VMEM((SUB, LANES), f32),
            pltpu.VMEM((2 * base, LANES), jnp.int32),
            pltpu.VMEM((nrow * per, LANES), f32),
            pltpu.VMEM((rings, dirs, n_band, 8, per, LANES), f32),
            pltpu.VMEM((n_band, SUB, LANES), f32),
            pltpu.VMEM((n_band, SUB, LANES), f32),
            pltpu.VMEM((n_band, SUB, LANES), f32),
            pltpu.VMEM((n_band * n_band if exchange else 1, SUB, LANES), f32),
            pltpu.VMEM(parts, f32),
            pltpu.VMEM(parts, f32),
            pltpu.VMEM(parts, f32),
            pltpu.VMEM(parts, f32),
            pltpu.VMEM((stations, 2 * base), bf16),
            pltpu.VMEM((2 * base, stations), bf16),
            pltpu.VMEM((PIECES * nrow, stations), bf16),
            pltpu.VMEM((PIECES * nrow, 2 * LANES), bf16),
            pltpu.VMEM((PIECES * 4 * dirs, 2 * base), bf16),
            pltpu.VMEM((nrow, 2 * base), f32),
            pltpu.VMEM((20 * dirs, base), f32),
            pltpu.VMEM((32 * dirs, base), f32),
            pltpu.VMEM((nrow, 2 * LANES), f32),
            pltpu.VMEM((4 * dirs, 2 * base), f32),
            pltpu.VMEM((nrow, stations), f32),
            pltpu.VMEM((nrow * per, LANES), f32),
            pltpu.VMEM((4 * dirs * per, LANES), f32),
            pltpu.VMEM((ITERS, chunks, 2) + piece, f32),
            pltpu.VMEM((ITERS, chunks) + piece, f32),
            pltpu.VMEM((ITERS, stages, chunks) + piece, f32),
            pltpu.VMEM((ITERS, max(1, stages - 1), chunks) + piece, f32),
            pltpu.VMEM((ITERS, chunks) + piece, f32),
            pltpu.VMEM((2,) + half, f32),
            pltpu.SemaphoreType.DMA((7,)),
            pltpu.SemaphoreType.DMA((1,)),
            pltpu.SemaphoreType.DMA((1,)),
            pltpu.SemaphoreType.DMA((2,)),
            pltpu.SemaphoreType.DMA((ITERS - 1, 2)),
            pltpu.SemaphoreType.DMA((1,)),
            pltpu.SemaphoreType.DMA((rings, dirs * ring_cuts(exchange), n_band - 1)),
            pltpu.SemaphoreType.DMA((stages + 1,)),
            pltpu.SemaphoreType.DMA((ITERS, stages + 1, chunks)),
        ],
        compiler_params=pltpu.CompilerParams(
            collective_id=0, has_side_effects=True, vmem_limit_bytes=56 * 1024 * 1024
        ),
    )(*[pltpu.with_memory_space_constraint(x, pltpu.HBM) for x in operands])
    jones, dual, coeffs = pl.pallas_call(
        flush,
        out_shape=(raw_out, raw_out, raw_terms),
        in_specs=[vmem] * 3,
        out_specs=(pl.BlockSpec(memory_space=pltpu.HBM),) * 3,
        scratch_shapes=[pltpu.SemaphoreType.DMA((3,))],
        compiler_params=pltpu.CompilerParams(vmem_limit_bytes=1024 * 1024),
    )(*[pltpu.with_memory_space_constraint(x, pltpu.VMEM) for x in results])
    return (
        leave(jones, jones_start.shape),
        leave(dual, jones_start.shape),
        leave(coeffs, consensus_start.shape),
    )


def solution(mesh):
    in_specs = (
        P("band", None, None, None, None, None),
        P("band", "dir", None, None, None, None, None),
        P("band", "dir", None, None, None, None),
        P("band", "dir", None, None, None, None),
        P(None, "dir", None, None, None, None),
        P("band", None),
        P(),
    )
    out_specs = (
        P("band", "dir", None, None, None, None),
        P("band", "dir", None, None, None, None),
        P(None, "dir", None, None, None, None),
    )
    body = functools.partial(local, mesh.shape["band"], mesh.shape["dir"])
    return jax.shard_map(body, mesh=mesh, in_specs=in_specs, out_specs=out_specs, check_vma=False)
```

```python
import functools

import jax
import jax.numpy as jnp
from jax import lax
from jax.experimental import pallas as pl
from jax.experimental.pallas import tpu as pltpu
from jax.sharding import PartitionSpec as P

ITERS = 3
RHO = 5.0
RIDGE = 0.25
LANES = 128
SUB = 8
PIECES = 3
ANSWER = 0
MESH = pl.DeviceIdType.MESH


def cmul(a, b):
    return (a[0] * b[0] - a[1] * b[1], a[0] * b[1] + a[1] * b[0])


def cmul_conj(a, b):
    return (a[0] * b[0] + a[1] * b[1], a[1] * b[0] - a[0] * b[1])


def cadd(a, b):
    return (a[0] + b[0], a[1] + b[1])


def conj(a):
    return (a[0], -a[1])


def re_mul(a, b):
    return a[0] * b[0] - a[1] * b[1]


def scale(r, a):
    return (r * a[0], r * a[1])


def split_store(ref, rows, value):
    left = value
    for piece in range(PIECES):
        part = left.astype(jnp.bfloat16)
        ref[piece * rows : (piece + 1) * rows, :] = part
        if piece + 1 < PIECES:
            left = left - part.astype(jnp.float32)


def join(value, rows):
    total = value[0:rows]
    for piece in range(1, PIECES):
        total = total + value[piece * rows : (piece + 1) * rows]
    return total


def kernel(
    n_band, n_dir, dirs, times, base, stations,
    vis_far, coh_far, jones0_far, dual0_far, coeffs0_far, basis_far, pairs_far,
    jones_out, dual_out, coeffs,
    vis, coh, jones0, dual0, coeffs0, basis, pairs_ref,
    jones, dual, row, ids_col,
    cons, xall, rows_all, weights, gweights, wmat,
    xs, inbox, outbox, consin,
    gather_hot, scatter_hot, lhs, lhs_c, lhs_n, ends, grams, cross, vals, vals_n, found, seg, seg_n,
    model, got_a, sums, got_b, got_c, res,
    greet_sem, load_sem, row_send, row_recv, p_send, p_recv, x_send, x_recv, d_send, d_recv,
):
    f32 = jnp.float32
    nrow = 8 * dirs
    per = stations // LANES
    me = lax.axis_index("band")
    mine = lax.axis_index("dir")
    chunks = base // LANES
    halves = times // SUB
    stages = n_dir.bit_length() - 1
    part_rows = nrow * per // n_band
    exchange = by_chunks(n_band, nrow * per)

    def at(pos):
        half = pos // (n_band // 2)
        return (1 - half) * (2 * pos) + half * (2 * (n_band - 1 - pos) + 1)

    odd = lax.rem(me, 2)
    pos = (1 - odd) * (me // 2) + odd * (n_band - 1 - me // 2)
    nexts = (at(lax.rem(pos + 1, n_band)), at(lax.rem(pos + n_band - 1, n_band)))

    def flip_bits(index, mask):
        out = index
        for b in range(mask.bit_length()):
            if mask >> b & 1:
                out = out + (1 - 2 * lax.rem(index // (1 << b), 2)) * (1 << b)
        return out

    def to_of(step):
        return flip_bits(me, step) if power_of_two(n_band) else lax.rem(me + step, n_band)

    def from_of(step):
        return flip_bits(me, step) if power_of_two(n_band) else lax.rem(me + n_band - step, n_band)

    def flip(stage):
        return flip_bits(mine, 1 << stage)

    def drain(ref, sem):
        pltpu.make_async_copy(ref, ref, sem).wait()

    own = lax.rem(mine, 2)
    leader = mine + 1 - own

    loads = {}
    for n, (name, source_ref, near) in enumerate((
        ("pairs", pairs_far, pairs_ref),
        ("jones", jones0_far, jones0),
        ("coh", coh_far, coh),
        ("basis", basis_far, basis),
        ("vis", vis_far, vis),
        ("dual", dual0_far, dual0),
        ("coeffs", coeffs0_far, coeffs0),
    )):
        loads[name] = pltpu.make_async_copy(source_ref, near, load_sem.at[n])
        loads[name].start()

    ways = min(2, n_band - 1)
    rounds = n_band // 2 - 1 if exchange else 0
    band_peers = list(nexts[:ways]) if exchange else [to_of(step) for step in range(1, n_band)]
    barrier = pltpu.get_barrier_semaphore()
    for peer in band_peers:
        pl.semaphore_signal(barrier, inc=1, device_id={"band": peer}, device_id_type=MESH)
    for stage in range(stages):
        pl.semaphore_signal(barrier, inc=1, device_id={"dir": flip(stage)}, device_id_type=MESH)

    def greet(r):
        if r < rounds:
            for way in range(ways):
                pl.semaphore_signal(
                    greet_sem.at[r], inc=1, device_id={"band": nexts[way]}, device_id_type=MESH
                )

    def hear(r):
        if r < rounds:
            pl.semaphore_wait(greet_sem.at[r], ways)
            greet(r + 1)

    def halves_of(k, v):
        return (k, v // 2, pl.ds(v % 2, per, stride=2), slice(None))

    def packed(k, v):
        return pl.ds((v * dirs + k) * per, per)

    def block_of(j):
        return j % 2, (j // 2) * LANES

    def gather_setup(c):
        step_rows = LANES

        def hot_body(i, carry):
            start = pl.multiple_of(i * step_rows, step_rows)
            sid = lax.broadcasted_iota(jnp.int32, (step_rows, LANES), 0) + i * step_rows
            for j in (2 * c, 2 * c + 1):
                lane = slice(j * LANES, (j + 1) * LANES)
                which, low = block_of(j)
                ids = pairs_ref[which : which + 1, low : low + LANES]
                same = sid == jnp.broadcast_to(ids, (step_rows, LANES))
                gather_hot[pl.ds(start, step_rows), lane] = jnp.where(same, 1.0, 0.0).astype(jnp.bfloat16)
            return carry

        lax.fori_loop(0, stations // step_rows, hot_body, 0)

    loads["pairs"].wait()
    group = 2 - chunks % 2
    for c in range(group):
        gather_setup(c)
    loads["jones"].wait()
    for k in range(dirs):
        for v in range(8):
            jones[packed(k, v), :] = jones0[halves_of(k, v)]

    def scatter_setup():
        step_rows = 32

        for j in range(2 * chunks):
            which, low = block_of(j)
            ids = jnp.broadcast_to(pairs_ref[which : which + 1, low : low + LANES], (LANES, LANES))
            ids_col[j * LANES : (j + 1) * LANES, :] = jnp.transpose(ids)

        def hot_body2(i, carry):
            start = pl.multiple_of(i * step_rows, step_rows)
            col = ids_col[pl.ds(start, step_rows), :]
            for j in range(stations // LANES):
                lane = slice(j * LANES, (j + 1) * LANES)
                sid = lax.broadcasted_iota(jnp.int32, (step_rows, LANES), 1) + j * LANES
                scatter_hot[pl.ds(start, step_rows), lane] = jnp.where(sid == col, 1.0, 0.0).astype(jnp.bfloat16)
            return carry

        lax.fori_loop(0, 2 * base // step_rows, hot_body2, 0)

    def first_sends():
        pl.semaphore_wait(barrier, len(band_peers) + stages)
        greet(0)
        loads["basis"].wait()
        row[...] = jnp.zeros((SUB, LANES), f32)
        for m in range(SUB):
            row[m : m + 1, :] = jnp.full((1, LANES), basis[0, m], f32)

    def send_rows():
        for step in range(1, n_band):
            pltpu.make_async_remote_copy(
                src_ref=row,
                dst_ref=rows_all.at[step],
                send_sem=row_send.at[0],
                recv_sem=row_recv.at[0],
                device_id={"band": to_of(step)},
                device_id_type=MESH,
            ).start()

    pairs = [(a, b) for a in range(4) for b in range(a, 4)]

    def gram_body(j, carry):
        lane = pl.ds(pl.multiple_of(j * LANES, LANES), LANES)
        for k in range(dirs):
            c = [
                [coh[k, v, h * SUB : (h + 1) * SUB, lane] for h in range(halves)]
                for v in range(8)
            ]
            for n, (a, b) in enumerate(pairs):
                real = sum(c[a][h] * c[b][h] + c[4 + a][h] * c[4 + b][h] for h in range(halves))
                grams[(2 * n) * dirs + k : (2 * n) * dirs + k + 1, lane] = jnp.sum(real, axis=0, keepdims=True)
                if a != b:
                    imag = sum(c[4 + a][h] * c[b][h] - c[a][h] * c[4 + b][h] for h in range(halves))
                    grams[(2 * n + 1) * dirs + k : (2 * n + 1) * dirs + k + 1, lane] = jnp.sum(
                        imag, axis=0, keepdims=True
                    )
        return carry

    def start_consensus():
        loads["coeffs"].wait()
        loads["dual"].wait()
        for k in range(dirs):
            for v in range(8):
                dual[packed(k, v), :] = dual0[halves_of(k, v)]
                total = basis[0, 0] * coeffs0[(0,) + halves_of(k, v)]
                for m in range(1, SUB):
                    total = total + basis[0, m] * coeffs0[(m,) + halves_of(k, v)]
                cons[packed(k, v), :] = total

    def solve_weights():
        drain(rows_all.at[pl.ds(1, n_band - 1)], row_recv.at[0])
        rows_all[0] = row[...]
        held = [rows_all[s] for s in range(n_band)]
        columns = []
        for m in range(SUB):
            total = held[0] * held[0][m : m + 1, :]
            for s in range(1, n_band):
                total = total + held[s] * held[s][m : m + 1, :]
            ident = jnp.where(lax.broadcasted_iota(jnp.int32, (SUB, LANES), 0) == m, RIDGE * n_band, 0.0)
            columns.append(total + ident.astype(f32))
        right = list(held)
        iota = lax.broadcasted_iota(jnp.int32, (SUB, LANES), 0)
        for i in range(SUB):
            inverse = 1.0 / columns[i][i : i + 1, :]
            factor = columns[i]
            for group in (columns, right):
                for c in range(len(group)):
                    lead = jnp.broadcast_to(group[c][i : i + 1, :] * inverse, (SUB, LANES))
                    group[c] = jnp.where(iota == i, lead, group[c] - factor * lead)

        def weight_of(a, b):
            return jnp.broadcast_to(jnp.sum(right[b] * held[a], axis=0, keepdims=True), (SUB, LANES))

        for s in range(n_band):
            band = from_of(s)
            gweights[band] = right[s]
            weights[band] = weight_of(0, s)
        if exchange:
            for a in range(n_band):
                for b in range(n_band):
                    wmat[a * n_band + b] = weight_of(a, b)

    x_copies = [{} for _ in range(ITERS)]
    ahead = n_band // 2
    behind = n_band - 1 - ahead

    def ring(turn):
        return 0 if exchange else turn

    def slot_of(way, distance):
        if distance > behind:
            return n_band - 1
        return distance + way * behind if distance else 0

    cuts = ring_cuts(exchange)
    units = dirs * cuts

    def reach_of(u, way):
        return ahead if way == u % 2 else behind

    order = [
        (u, way)
        for pair in zip(*[sorted(range(units), key=lambda u: -reach_of(u, way)) for way in range(2)])
        for way, u in enumerate(pair)
    ]

    def send_x(turn, u, way, distance):
        to = slot_of(way, distance + 1)
        k, rows = u // cuts, pl.ds(u % cuts * (8 // cuts), 8 // cuts)
        copy = pltpu.make_async_remote_copy(
            src_ref=xall.at[ring(turn), k, slot_of(way, distance), rows],
            dst_ref=xall.at[ring(turn), k, to, rows],
            send_sem=x_send.at[0],
            recv_sem=x_recv.at[ring(turn), u, to - 1],
            device_id={"band": nexts[way]},
            device_id_type=MESH,
        )
        copy.start()
        x_copies[turn][(u, way, distance + 1)] = copy

    def pump(turn, distance):
        for u, way in order:
            reach = reach_of(u, way)
            if distance <= reach:
                x_copies[turn][(u, way, distance)].wait_recv()
                if distance < reach:
                    send_x(turn, u, way, distance)

    def source(slot):
        if slot <= behind:
            return at(lax.rem(pos + n_band - slot, n_band))
        return at(lax.rem(pos + slot - behind, n_band))

    def part_of(k, v):
        here = (v * dirs + k) * per
        return here // part_rows, pl.ds(here % part_rows, per)

    def send_parts(turn):
        for step in range(n_band - 1, 0, -1):
            pltpu.make_async_remote_copy(
                src_ref=xs.at[turn, to_of(step)],
                dst_ref=inbox.at[turn, own, step],
                send_sem=p_send.at[0],
                recv_sem=p_recv.at[turn, own],
                device_id={"band": to_of(step), "dir": leader},
                device_id_type=MESH,
            ).start()

        @pl.when(own == 0)
        def _():
            pltpu.make_async_remote_copy(
                src_ref=xs.at[turn, me],
                dst_ref=inbox.at[turn, 0, 0],
                send_sem=p_send.at[0],
                recv_sem=p_recv.at[turn, 0],
                device_id={"dir": flip(0)},
                device_id_type=MESH,
            ).start()

        @pl.when(own == 1)
        def _():
            inbox[turn, 1, 0] = xs[turn, me]

    def answer_parts(turn, side):
        if side == 0:
            drain(inbox.at[turn, 0], p_recv.at[turn, 0])
        else:
            drain(inbox.at[turn, 1, pl.ds(1, n_band - 1)], p_recv.at[turn, 1])
        for a in range(n_band - 1, -1, -1):
            for r in range(part_rows // SUB):
                here = slice(r * SUB, (r + 1) * SUB)
                total = wmat[a * n_band] * inbox[turn, side, 0, here, :]
                for b in range(1, n_band):
                    total = total + wmat[a * n_band + b] * inbox[turn, side, b, here, :]
                outbox[turn, side, a, here, :] = total
            if a or side == 0:
                pltpu.make_async_remote_copy(
                    src_ref=outbox.at[turn, side, a],
                    dst_ref=consin.at[turn, me],
                    send_sem=p_send.at[1],
                    recv_sem=p_recv.at[turn, 2],
                    device_id={"band": to_of(a), "dir": flip(0)} if side == 0 else {"band": to_of(a)},
                    device_id_type=MESH,
                ).start()

    def send_d(turn, n, c):
        if n == 0:
            src, dst = model.at[turn, c], got_a.at[turn, c]
        elif n < stages:
            src, dst = sums.at[turn, n - 1, c], got_b.at[turn, n - 1, c]
        else:
            src, dst = sums.at[turn, stages - 1, c], got_c.at[turn, c]
        return pltpu.make_async_remote_copy(
            src_ref=src,
            dst_ref=dst,
            send_sem=d_send.at[n],
            recv_sem=d_recv.at[turn, n, c],
            device_id={"dir": flip(n if n < stages else 0)},
            device_id_type=MESH,
        )

    def end(comp, lane):
        return ends[comp * dirs : (comp + 1) * dirs, lane]

    def gram(a, b, lane):
        if a > b:
            return conj(gram(b, a, lane))
        n = pairs.index((a, b))
        real = grams[(2 * n) * dirs : (2 * n + 1) * dirs, lane]
        if a == b:
            return real
        return (real, grams[(2 * n + 1) * dirs : (2 * n + 2) * dirs, lane])

    def first_of(c):
        return slice(2 * c * LANES, (2 * c + 1) * LANES)

    def second_of(c):
        return slice((2 * c + 1) * LANES, (2 * c + 2) * LANES)

    def chunk_of(c):
        return slice(c * LANES, (c + 1) * LANES)

    for turn in range(ITERS):
        for g in range(nrow // SUB):
            for j in range(per):
                left = jones[pl.ds(g * SUB * per + j, SUB, stride=per), :]
                for piece in range(PIECES):
                    part = left.astype(jnp.bfloat16)
                    lhs[
                        piece * nrow + g * SUB : piece * nrow + (g + 1) * SUB,
                        j * LANES : (j + 1) * LANES,
                    ] = part
                    left = left - part.astype(f32)

        def gather(c):
            lane = slice(2 * c * LANES, 2 * (c + group) * LANES)
            ends[:, lane] = join(jnp.dot(lhs[...], gather_hot[:, lane], preferred_element_type=f32), nrow)

        def predict(c):
            lane, lane_p, lane_q = chunk_of(c), first_of(c), second_of(c)

            def model_body(h, carry):
                time = pl.ds(pl.multiple_of(h * SUB, SUB), SUB)
                total = [None] * 4
                for k in range(dirs):
                    co = [(coh[k, v, time, lane], coh[k, 4 + v, time, lane]) for v in range(4)]

                    def spread(v, where):
                        return tuple(
                            jnp.broadcast_to(
                                ends[(4 * part + v) * dirs + k : (4 * part + v) * dirs + k + 1, where],
                                (SUB, LANES),
                            )
                            for part in range(2)
                        )

                    p = [spread(v, lane_p) for v in range(4)]
                    q = [spread(v, lane_q) for v in range(4)]
                    for a in range(2):
                        b = [cadd(cmul(p[2 * a], co[d]), cmul(p[2 * a + 1], co[2 + d])) for d in range(2)]
                        for d in range(2):
                            term = cadd(cmul_conj(b[0], q[2 * d]), cmul_conj(b[1], q[2 * d + 1]))
                            v = 2 * a + d
                            total[v] = term if total[v] is None else cadd(total[v], term)
                for v in range(4):
                    model[turn, c, 0, v, time, :] = total[v][0]
                    model[turn, c, 1, v, time, :] = total[v][1]
                return carry

            lax.fori_loop(0, halves, model_body, 0)

        for c in range(chunks):
            if c % group == 0:
                if turn == 0 and c > 0:
                    for e in range(group):
                        gather_setup(c + e)
                gather(c)
            if turn == 0 and c == 0:
                loads["coh"].wait()
            predict(c)
            if turn == 0 and c == 0:
                first_sends()

            @pl.when(own == 0)
            def _():
                send_d(turn, 0, c).start()

        def collect(c):
            send_d(turn, 0, c).wait_recv()
            sums[turn, 0, c] = model[turn, c] + got_a[turn, c]
            if stages > 1:
                send_d(turn, 1, c).start()

        def collect_next(stage, c):
            send_d(turn, stage, c).wait_recv()
            sums[turn, stage, c] = sums[turn, stage - 1, c] + got_b[turn, stage - 1, c]
            if stage + 1 < stages:
                send_d(turn, stage + 1, c).start()

        def obtain(c):
            lane = chunk_of(c)

            @pl.when(own == 1)
            def _():
                if stages > 1:
                    collect_next(stages - 1, c)
                send_d(turn, stages, c).start()
                res[:, :, :, lane] = vis[:, :, :, lane] - sums[turn, stages - 1, c]

            @pl.when(own == 0)
            def _():
                send_d(turn, stages, c).wait_recv()
                res[:, :, :, lane] = vis[:, :, :, lane] - got_c[turn, c]

        def gram_of(j):
            m00 = re_mul(j[0], conj(j[0])) + re_mul(j[2], conj(j[2]))
            m11 = re_mul(j[1], conj(j[1])) + re_mul(j[3], conj(j[3]))
            m01 = cadd(cmul_conj(j[1], j[0]), cmul_conj(j[3], j[2]))
            return m00, m11, m01

        def ends_of(lane):
            return [(end(v, lane), end(4 + v, lane)) for v in range(4)]

        def normals(c):
            lane = chunk_of(c)

            def gr(a, b):
                return gram(a, b, lane)

            jp, jq = ends_of(first_of(c)), ends_of(second_of(c))
            m00, m11, m01 = gram_of(jq)
            p00, p11, p01 = gram_of(jp)
            n1_00 = m00 * gr(0, 0) + m11 * gr(1, 1) + 2.0 * re_mul(m01, gr(0, 1))
            n1_11 = m00 * gr(2, 2) + m11 * gr(3, 3) + 2.0 * re_mul(m01, gr(2, 3))
            n1_01 = cadd(
                cadd(scale(m00, gr(0, 2)), scale(m11, gr(1, 3))),
                cadd(cmul(m01, gr(0, 3)), cmul(conj(m01), gr(1, 2))),
            )
            n2_00 = p00 * gr(0, 0) + p11 * gr(2, 2) + 2.0 * re_mul(p01, gr(2, 0))
            n2_11 = p00 * gr(1, 1) + p11 * gr(3, 3) + 2.0 * re_mul(p01, gr(3, 1))
            n2_01 = cadd(
                cadd(scale(p00, gr(1, 0)), scale(p11, gr(3, 2))),
                cadd(cmul(p01, gr(3, 0)), cmul(conj(p01), gr(1, 2))),
            )
            for n, (left, right) in enumerate(
                ((n1_00, n2_00), (n1_11, n2_11), (n1_01[0], n2_01[0]), (n1_01[1], n2_01[1]))
            ):
                vals_n[n * dirs : (n + 1) * dirs, first_of(c)] = left
                vals_n[n * dirs : (n + 1) * dirs, second_of(c)] = right

        def scatter_normals():
            split_store(lhs_n, 4 * dirs, vals_n[...])
            out = join(jnp.dot(lhs_n[...], scatter_hot[...], preferred_element_type=f32), 4 * dirs)
            for g in range(4 * dirs // SUB):
                for j in range(per):
                    seg_n[pl.ds(g * SUB * per + j, SUB, stride=per), :] = out[
                        g * SUB : (g + 1) * SUB, j * LANES : (j + 1) * LANES
                    ]

        def finish(c):
            lane = chunk_of(c)
            r = [[res[v // 4, v % 4, h * SUB : (h + 1) * SUB, lane] for h in range(halves)] for v in range(8)]
            for k in range(dirs):
                co = [[coh[k, v, h * SUB : (h + 1) * SUB, lane] for h in range(halves)] for v in range(8)]
                for a in range(4):
                    for b in range(4):
                        real = sum(r[a][h] * co[b][h] + r[4 + a][h] * co[4 + b][h] for h in range(halves))
                        imag = sum(r[4 + a][h] * co[b][h] - r[a][h] * co[4 + b][h] for h in range(halves))
                        n = 2 * (4 * a + b)
                        cross[n * dirs + k : n * dirs + k + 1, lane] = jnp.sum(real, axis=0, keepdims=True)
                        cross[(n + 1) * dirs + k : (n + 1) * dirs + k + 1, lane] = jnp.sum(
                            imag, axis=0, keepdims=True
                        )

            def crossed(a, b):
                n = 2 * (4 * a + b)
                return (
                    cross[n * dirs : (n + 1) * dirs, lane],
                    cross[(n + 1) * dirs : (n + 2) * dirs, lane],
                )

            jp, jq = ends_of(first_of(c)), ends_of(second_of(c))
            for which, j, other_end in ((0, jq, jp), (1, jp, jq)):
                where = second_of(c) if which else first_of(c)
                h00, h11, re01, im01 = [vals_n[n * dirs : (n + 1) * dirs, where] for n in range(4)]
                h01 = (re01, im01)
                for a in range(2):
                    for d in range(2):
                        total = None
                        for b in range(2):
                            for e in range(2):
                                if which == 0:
                                    term = cmul(j[2 * b + e], crossed(2 * a + b, 2 * d + e))
                                else:
                                    term = cmul_conj(j[2 * b + e], crossed(2 * b + a, 2 * e + d))
                                total = term if total is None else cadd(total, term)
                        if d == 0:
                            extra = cadd(scale(h00, other_end[2 * a]), cmul_conj(other_end[2 * a + 1], h01))
                        else:
                            extra = cadd(cmul(other_end[2 * a], h01), scale(h11, other_end[2 * a + 1]))
                        total = cadd(total, extra)
                        for part in range(2):
                            n = 4 * part + 2 * a + d
                            vals[n * dirs : (n + 1) * dirs, which * LANES : (which + 1) * LANES] = total[part]

            split_store(lhs_c, nrow, vals[...])
            rows = slice(2 * c * LANES, (2 * c + 2) * LANES)
            out = join(jnp.dot(lhs_c[...], scatter_hot[rows, :], preferred_element_type=f32), nrow)
            if c > 0:
                out = out + found[...]
            if c + 1 < chunks:
                found[...] = out
            else:
                for g in range(nrow // SUB):
                    for j in range(per):
                        seg[pl.ds(g * SUB * per + j, SUB, stride=per), :] = out[
                            g * SUB : (g + 1) * SUB, j * LANES : (j + 1) * LANES
                        ]

        if turn == 0:
            lax.fori_loop(0, chunks, gram_body, 0)
        if turn > 0:
            for c in range(chunks):
                normals(c)
            scatter_normals()

        @pl.when(own == 1)
        def _():
            for c in range(chunks):
                collect(c)

        if turn == 0:
            for c in range(chunks):
                normals(c)
            hear(0)
            scatter_setup()
            scatter_normals()
            start_consensus()
            hear(1)
            loads["vis"].wait()
        if turn > 0 and exchange:

            @pl.when(own == 1)
            def _():
                if turn == 1:
                    solve_weights()
                answer_parts(turn - 1, 1)

            if turn == 2:

                @pl.when(own == 0)
                def _():
                    solve_weights()

        if turn == 1 and not exchange:
            solve_weights()
        if stages > 2:

            @pl.when(own == 1)
            def _():
                for stage in range(1, stages - 1):
                    for c in range(chunks):
                        collect_next(stage, c)

        for c in range(chunks):
            obtain(c)
            if turn > 0 and exchange and c == ANSWER:

                @pl.when(own == 1)
                def _():
                    answer_parts(turn - 1, 0)

            finish(c)
            if turn == 0 and c == min(1, chunks - 1):
                for r in range(2, max(2, rounds)):
                    hear(r)
                send_rows()

        def refresh(k, v, total, previous):
            here = packed(k, v)
            fresh = dual[here, :] + RHO * (jones[here, :] - total)
            if previous + 1 < ITERS:
                cons[here, :] = total
                dual[here, :] = fresh
            else:
                dual_out[halves_of(k, v)] = fresh

        def join_parts(previous):
            @pl.when(own == 0)
            def _():
                drain(consin.at[previous], p_recv.at[previous, 2])

            @pl.when(own == 1)
            def _():
                drain(consin.at[previous, pl.ds(1, n_band - 1)], p_recv.at[previous, 2])
                consin[previous, me] = outbox[previous, 1, 0]

            for k in range(dirs):
                for v in range(8):
                    part, rows = part_of(k, v)
                    refresh(k, v, consin[previous, part, rows, :], previous)

        def ring_sum(turn, k, v, slots, total=None):
            for s in slots:
                term = weights[source(s)] * xall[ring(turn), k, s, v]
                total = term if total is None else total + term
            return total

        if turn > 0:
            if exchange:
                join_parts(turn - 1)
            else:
                for s in range(1, ahead + 1):
                    pump(turn - 1, s)
                for k in range(dirs):
                    for v in range(8):
                        refresh(k, v, ring_sum(turn - 1, k, v, range(n_band)), turn - 1)

        by_ring = turn + 1 == ITERS or not exchange
        for k in range(dirs):
            y = []
            for v in range(8):
                here = packed(k, v)
                y.append(seg[here, :] + RHO * cons[here, :] - dual[here, :])
            h00, h11, re01, im01 = [seg_n[packed(k, n), :] for n in range(4)]
            h00 = h00 + RHO
            h11 = h11 + RHO
            inverse = 1.0 / (h00 * h11 - (re01 * re01 + im01 * im01))
            h00, h11, h01 = h00 * inverse, h11 * inverse, (re01 * inverse, im01 * inverse)
            for a in range(2):
                y0, y1 = (y[2 * a], y[4 + 2 * a]), (y[2 * a + 1], y[4 + 2 * a + 1])
                minus0, minus1 = cmul_conj(y1, h01), cmul(y0, h01)
                for part in range(2):
                    for c in range(2):
                        if c == 0:
                            value = h11 * y0[part] - minus0[part]
                        else:
                            value = h00 * y1[part] - minus1[part]
                        v = 4 * part + 2 * a + c
                        here = packed(k, v)
                        jones[here, :] = value
                        if turn + 1 == ITERS:
                            jones_out[halves_of(k, v)] = value
                        sent = value + dual[here, :] * (1.0 / RHO)
                        if by_ring:
                            xall[ring(turn), k, 0, v] = sent
                        else:
                            chunk, rows = part_of(k, v)
                            xs[turn, chunk, rows, :] = sent
        if by_ring:
            for u, way in order:
                if reach_of(u, way):
                    send_x(turn, u, way, 0)
        else:
            send_parts(turn)

    last = ITERS - 1
    for s in range(1, ahead):
        pump(last, s)

    def coeff_body(slots, first):
        def run(m, carry):
            for k in range(dirs):
                total = [None] * 8 if first else [coeffs[(m,) + halves_of(k, v)] for v in range(8)]
                for s in slots:
                    factor = jnp.broadcast_to(gweights[source(s), pl.ds(m, 1), :], (SUB, LANES))
                    for v in range(8):
                        term = factor * xall[ring(last), k, s, v]
                        total[v] = term if total[v] is None else total[v] + term
                for v in range(8):
                    coeffs[(m,) + halves_of(k, v)] = total[v]
            return carry

        lax.fori_loop(0, SUB, run, 0)

    early = range(n_band - 1)
    coeff_body(early, True)
    for k in range(dirs):
        for v in range(8):
            cons[packed(k, v), :] = ring_sum(last, k, v, early)
    pump(last, ahead)
    late = range(n_band - 1, n_band)
    for k in range(dirs):
        for v in range(8):
            refresh(k, v, ring_sum(last, k, v, late, cons[packed(k, v), :]), last)
    coeff_body(late, False)

    drain(rows_all.at[pl.ds(1, n_band - 1)], row_send.at[0])
    drain(xall.at[:, :, pl.ds(1, n_band - 1)], x_send.at[0])

    @pl.when(own == 0)
    def _():
        drain(model, d_send.at[0])
        if exchange:
            drain(xs, p_send.at[0])

    @pl.when(own == 1)
    def _():
        for n in range(1, stages + 1):
            drain(model, d_send.at[n])
        if exchange:
            drain(inbox.at[:, 1, pl.ds(1, n_band - 1)], p_send.at[0])
            drain(inbox.at[:, 0], p_send.at[1])
            drain(inbox.at[:, 1, pl.ds(1, n_band - 1)], p_send.at[1])


def flush(*refs):
    count = (len(refs) - 1) // 2
    sem = refs[-1]
    copies = [pltpu.make_async_copy(refs[n], refs[count + n], sem.at[n]) for n in range(count)]
    for copy in copies:
        copy.start()
    for copy in copies:
        copy.wait()


def power_of_two(n):
    return n & (n - 1) == 0


def ring_cuts(exchange):
    return 2 if exchange else 1


def by_chunks(n_band, rows):
    return power_of_two(n_band) and rows % (n_band * SUB) == 0


def local(n_band, n_dir, vis, coh, jones_start, dual_start, consensus_start, freq_basis, pairs):
    f32 = jnp.float32
    dirs, times, base = coh.shape[1], coh.shape[-2], coh.shape[-1]
    stations = jones_start.shape[-1]
    per = stations // LANES
    nrow = 8 * dirs
    terms = freq_basis.shape[1]

    def enter(value):
        lead = value.shape[:-2]
        value = value.reshape(lead + (2, per, LANES))
        return jnp.swapaxes(value, -2, -3).reshape(lead + (2 * per, LANES))

    def leave(value, shape):
        value = value.reshape(value.shape[:-2] + (per, 2, LANES))
        return jnp.swapaxes(value, -2, -3).reshape(shape)

    stages = n_dir.bit_length() - 1
    chunks = base // LANES
    exchange = by_chunks(n_band, nrow * per)
    rings = 1 if exchange else ITERS
    parts = (ITERS - 1, n_band, max(SUB, nrow * per // n_band), LANES) if exchange else (1, 1, SUB, LANES)
    half = (4, times, base)
    piece = (2, 4, times, LANES)
    vmem = pl.BlockSpec(memory_space=pltpu.VMEM)
    far = pl.BlockSpec(memory_space=pltpu.HBM)
    raw = (dirs, 4, 2 * per, LANES)
    raw_out = jax.ShapeDtypeStruct(raw, f32)
    raw_terms = jax.ShapeDtypeStruct((terms,) + raw, f32)
    bf16 = jnp.bfloat16
    operands = (
        vis.reshape((2,) + half),
        coh.reshape(dirs, 8, times, base),
        enter(jones_start.reshape((dirs, 4, 2, stations))),
        enter(dual_start.reshape((dirs, 4, 2, stations))),
        enter(consensus_start.reshape((terms, dirs, 4, 2, stations))),
        freq_basis,
        pairs,
    )
    results = pl.pallas_call(
        functools.partial(kernel, n_band, n_dir, dirs, times, base, stations),
        out_shape=(pltpu.VMEM(raw, f32), pltpu.VMEM(raw, f32), pltpu.VMEM((terms,) + raw, f32)),
        in_specs=[far] * 7,
        out_specs=(vmem,) * 3,
        scratch_shapes=[
            pltpu.VMEM((2,) + half, f32),
            pltpu.VMEM((dirs, 8, times, base), f32),
            pltpu.VMEM(raw, f32),
            pltpu.VMEM(raw, f32),
            pltpu.VMEM((terms,) + raw, f32),
            pltpu.SMEM(freq_basis.shape, f32),
            pltpu.VMEM((2, base), jnp.int32),
            pltpu.VMEM((nrow * per, LANES), f32),
            pltpu.VMEM((nrow * per, LANES), f32),
            pltpu.VMEM((SUB, LANES), f32),
            pltpu.VMEM((2 * base, LANES), jnp.int32),
            pltpu.VMEM((nrow * per, LANES), f32),
            pltpu.VMEM((rings, dirs, n_band, 8, per, LANES), f32),
            pltpu.VMEM((n_band, SUB, LANES), f32),
            pltpu.VMEM((n_band, SUB, LANES), f32),
            pltpu.VMEM((n_band, SUB, LANES), f32),
            pltpu.VMEM((n_band * n_band if exchange else 1, SUB, LANES), f32),
            pltpu.VMEM(parts, f32),
            pltpu.VMEM(parts[:1] + (2,) + parts[1:], f32),
            pltpu.VMEM(parts[:1] + (2,) + parts[1:], f32),
            pltpu.VMEM(parts, f32),
            pltpu.VMEM((stations, 2 * base), bf16),
            pltpu.VMEM((2 * base, stations), bf16),
            pltpu.VMEM((PIECES * nrow, stations), bf16),
            pltpu.VMEM((PIECES * nrow, 2 * LANES), bf16),
            pltpu.VMEM((PIECES * 4 * dirs, 2 * base), bf16),
            pltpu.VMEM((nrow, 2 * base), f32),
            pltpu.VMEM((20 * dirs, base), f32),
            pltpu.VMEM((32 * dirs, base), f32),
            pltpu.VMEM((nrow, 2 * LANES), f32),
            pltpu.VMEM((4 * dirs, 2 * base), f32),
            pltpu.VMEM((nrow, stations), f32),
            pltpu.VMEM((nrow * per, LANES), f32),
            pltpu.VMEM((4 * dirs * per, LANES), f32),
            pltpu.VMEM((ITERS, chunks) + piece, f32),
            pltpu.VMEM((ITERS, chunks) + piece, f32),
            pltpu.VMEM((ITERS, stages, chunks) + piece, f32),
            pltpu.VMEM((ITERS, max(1, stages - 1), chunks) + piece, f32),
            pltpu.VMEM((ITERS, chunks) + piece, f32),
            pltpu.VMEM((2,) + half, f32),
            pltpu.SemaphoreType.REGULAR((max(1, n_band // 2 - 1) if exchange else 1,)),
            pltpu.SemaphoreType.DMA((7,)),
            pltpu.SemaphoreType.DMA((1,)),
            pltpu.SemaphoreType.DMA((1,)),
            pltpu.SemaphoreType.DMA((2,)),
            pltpu.SemaphoreType.DMA((ITERS - 1, 3)),
            pltpu.SemaphoreType.DMA((1,)),
            pltpu.SemaphoreType.DMA((rings, dirs * ring_cuts(exchange), n_band - 1)),
            pltpu.SemaphoreType.DMA((stages + 1,)),
            pltpu.SemaphoreType.DMA((ITERS, stages + 1, chunks)),
        ],
        compiler_params=pltpu.CompilerParams(
            collective_id=0, has_side_effects=True, vmem_limit_bytes=56 * 1024 * 1024
        ),
    )(*[pltpu.with_memory_space_constraint(x, pltpu.HBM) for x in operands])
    jones, dual, coeffs = pl.pallas_call(
        flush,
        out_shape=(raw_out, raw_out, raw_terms),
        in_specs=[vmem] * 3,
        out_specs=(pl.BlockSpec(memory_space=pltpu.HBM),) * 3,
        scratch_shapes=[pltpu.SemaphoreType.DMA((3,))],
        compiler_params=pltpu.CompilerParams(vmem_limit_bytes=1024 * 1024),
    )(*[pltpu.with_memory_space_constraint(x, pltpu.VMEM) for x in results])
    return (
        leave(jones, jones_start.shape),
        leave(dual, jones_start.shape),
        leave(coeffs, consensus_start.shape),
    )


def solution(mesh):
    in_specs = (
        P("band", None, None, None, None, None),
        P("band", "dir", None, None, None, None, None),
        P("band", "dir", None, None, None, None),
        P("band", "dir", None, None, None, None),
        P(None, "dir", None, None, None, None),
        P("band", None),
        P(),
    )
    out_specs = (
        P("band", "dir", None, None, None, None),
        P("band", "dir", None, None, None, None),
        P(None, "dir", None, None, None, None),
    )
    body = functools.partial(local, mesh.shape["band"], mesh.shape["dir"])
    return jax.shard_map(body, mesh=mesh, in_specs=in_specs, out_specs=out_specs, check_vma=False)
```

```python
import functools

import jax
import jax.numpy as jnp
from jax import lax
from jax.experimental import pallas as pl
from jax.experimental.pallas import tpu as pltpu
from jax.sharding import PartitionSpec as P

ITERS = 3
RHO = 5.0
RIDGE = 0.25
LANES = 128
SUB = 8
PIECES = 3
ANSWER = 0
MESH = pl.DeviceIdType.MESH


def cmul(a, b):
    return (a[0] * b[0] - a[1] * b[1], a[0] * b[1] + a[1] * b[0])


def cmul_conj(a, b):
    return (a[0] * b[0] + a[1] * b[1], a[1] * b[0] - a[0] * b[1])


def cadd(a, b):
    return (a[0] + b[0], a[1] + b[1])


def conj(a):
    return (a[0], -a[1])


def re_mul(a, b):
    return a[0] * b[0] - a[1] * b[1]


def scale(r, a):
    return (r * a[0], r * a[1])


def split_store(ref, rows, value):
    left = value
    for piece in range(PIECES):
        part = left.astype(jnp.bfloat16)
        ref[piece * rows : (piece + 1) * rows, :] = part
        if piece + 1 < PIECES:
            left = left - part.astype(jnp.float32)


def join(value, rows):
    total = value[0:rows]
    for piece in range(1, PIECES):
        total = total + value[piece * rows : (piece + 1) * rows]
    return total


def kernel(
    n_band, n_dir, dirs, times, base, stations,
    vis_far, coh_far, jones0_far, dual0_far, coeffs0_far, basis_far, pairs_far,
    jones_out, dual_out, coeffs,
    vis, coh, jones0, dual0, coeffs0, basis, pairs_ref,
    jones, dual, row, ids_col,
    cons, xall, rows_all, weights, gweights, wmat,
    xs, inbox, outbox, consin,
    gather_hot, scatter_hot, lhs, lhs_c, lhs_n, ends, grams, cross, vals, vals_n, found, seg, seg_n,
    model, got_a, sums, got_b, got_c, res,
    greet_sem, load_sem, row_send, row_recv, p_send, p_recv, x_send, x_recv, x_far, d_send, d_recv,
):
    f32 = jnp.float32
    nrow = 8 * dirs
    per = stations // LANES
    me = lax.axis_index("band")
    mine = lax.axis_index("dir")
    chunks = base // LANES
    halves = times // SUB
    stages = n_dir.bit_length() - 1
    part_rows = nrow * per // n_band
    exchange = by_chunks(n_band, nrow * per)

    def at(pos):
        half = pos // (n_band // 2)
        return (1 - half) * (2 * pos) + half * (2 * (n_band - 1 - pos) + 1)

    odd = lax.rem(me, 2)
    pos = (1 - odd) * (me // 2) + odd * (n_band - 1 - me // 2)
    nexts = (at(lax.rem(pos + 1, n_band)), at(lax.rem(pos + n_band - 1, n_band)))

    def flip_bits(index, mask):
        out = index
        for b in range(mask.bit_length()):
            if mask >> b & 1:
                out = out + (1 - 2 * lax.rem(index // (1 << b), 2)) * (1 << b)
        return out

    def to_of(step):
        return flip_bits(me, step) if power_of_two(n_band) else lax.rem(me + step, n_band)

    def from_of(step):
        return flip_bits(me, step) if power_of_two(n_band) else lax.rem(me + n_band - step, n_band)

    def flip(stage):
        return flip_bits(mine, 1 << stage)

    def drain(ref, sem):
        pltpu.make_async_copy(ref, ref, sem).wait()

    own = lax.rem(mine, 2)
    leader = mine + 1 - own

    loads = {}
    for n, (name, source_ref, near) in enumerate((
        ("pairs", pairs_far, pairs_ref),
        ("jones", jones0_far, jones0),
        ("coh", coh_far, coh),
        ("basis", basis_far, basis),
        ("vis", vis_far, vis),
        ("dual", dual0_far, dual0),
        ("coeffs", coeffs0_far, coeffs0),
    )):
        loads[name] = pltpu.make_async_copy(source_ref, near, load_sem.at[n])
        loads[name].start()

    ways = min(2, n_band - 1)
    rounds = n_band // 2 - 1 if exchange else 0
    band_peers = list(nexts[:ways]) if exchange else [to_of(step) for step in range(1, n_band)]
    barrier = pltpu.get_barrier_semaphore()
    for peer in band_peers:
        pl.semaphore_signal(barrier, inc=1, device_id={"band": peer}, device_id_type=MESH)
    for stage in range(stages):
        pl.semaphore_signal(barrier, inc=1, device_id={"dir": flip(stage)}, device_id_type=MESH)

    def greet(r):
        if r < rounds:
            for way in range(ways):
                pl.semaphore_signal(
                    greet_sem.at[r], inc=1, device_id={"band": nexts[way]}, device_id_type=MESH
                )

    def hear(r):
        if r < rounds:
            pl.semaphore_wait(greet_sem.at[r], ways)
            greet(r + 1)

    def halves_of(k, v):
        return (k, v // 2, pl.ds(v % 2, per, stride=2), slice(None))

    def packed(k, v):
        return pl.ds((v * dirs + k) * per, per)

    def block_of(j):
        return j % 2, (j // 2) * LANES

    def gather_setup(c):
        step_rows = LANES

        def hot_body(i, carry):
            start = pl.multiple_of(i * step_rows, step_rows)
            sid = lax.broadcasted_iota(jnp.int32, (step_rows, LANES), 0) + i * step_rows
            for j in (2 * c, 2 * c + 1):
                lane = slice(j * LANES, (j + 1) * LANES)
                which, low = block_of(j)
                ids = pairs_ref[which : which + 1, low : low + LANES]
                same = sid == jnp.broadcast_to(ids, (step_rows, LANES))
                gather_hot[pl.ds(start, step_rows), lane] = jnp.where(same, 1.0, 0.0).astype(jnp.bfloat16)
            return carry

        lax.fori_loop(0, stations // step_rows, hot_body, 0)

    loads["pairs"].wait()
    group = 2 - chunks % 2
    gather_setup(0)
    loads["jones"].wait()
    for k in range(dirs):
        for v in range(8):
            jones[packed(k, v), :] = jones0[halves_of(k, v)]

    def scatter_setup():
        step_rows = 32

        for j in range(2 * chunks):
            which, low = block_of(j)
            ids = jnp.broadcast_to(pairs_ref[which : which + 1, low : low + LANES], (LANES, LANES))
            ids_col[j * LANES : (j + 1) * LANES, :] = jnp.transpose(ids)

        def hot_body2(i, carry):
            start = pl.multiple_of(i * step_rows, step_rows)
            col = ids_col[pl.ds(start, step_rows), :]
            for j in range(stations // LANES):
                lane = slice(j * LANES, (j + 1) * LANES)
                sid = lax.broadcasted_iota(jnp.int32, (step_rows, LANES), 1) + j * LANES
                scatter_hot[pl.ds(start, step_rows), lane] = jnp.where(sid == col, 1.0, 0.0).astype(jnp.bfloat16)
            return carry

        lax.fori_loop(0, 2 * base // step_rows, hot_body2, 0)

    def first_sends():
        pl.semaphore_wait(barrier, len(band_peers) + stages)
        greet(0)
        loads["basis"].wait()
        row[...] = jnp.zeros((SUB, LANES), f32)
        for m in range(SUB):
            row[m : m + 1, :] = jnp.full((1, LANES), basis[0, m], f32)

    def send_rows():
        for step in range(1, n_band):
            pltpu.make_async_remote_copy(
                src_ref=row,
                dst_ref=rows_all.at[step],
                send_sem=row_send.at[0],
                recv_sem=row_recv.at[0],
                device_id={"band": to_of(step)},
                device_id_type=MESH,
            ).start()

    pairs = [(a, b) for a in range(4) for b in range(a, 4)]

    def gram_body(j, carry):
        lane = pl.ds(pl.multiple_of(j * LANES, LANES), LANES)
        for k in range(dirs):
            c = [
                [coh[k, v, h * SUB : (h + 1) * SUB, lane] for h in range(halves)]
                for v in range(8)
            ]
            for n, (a, b) in enumerate(pairs):
                real = sum(c[a][h] * c[b][h] + c[4 + a][h] * c[4 + b][h] for h in range(halves))
                grams[(2 * n) * dirs + k : (2 * n) * dirs + k + 1, lane] = jnp.sum(real, axis=0, keepdims=True)
                if a != b:
                    imag = sum(c[4 + a][h] * c[b][h] - c[a][h] * c[4 + b][h] for h in range(halves))
                    grams[(2 * n + 1) * dirs + k : (2 * n + 1) * dirs + k + 1, lane] = jnp.sum(
                        imag, axis=0, keepdims=True
                    )
        return carry

    def start_consensus():
        loads["coeffs"].wait()
        loads["dual"].wait()
        for k in range(dirs):
            for v in range(8):
                dual[packed(k, v), :] = dual0[halves_of(k, v)]
                total = basis[0, 0] * coeffs0[(0,) + halves_of(k, v)]
                for m in range(1, SUB):
                    total = total + basis[0, m] * coeffs0[(m,) + halves_of(k, v)]
                cons[packed(k, v), :] = total

    def solve_weights():
        drain(rows_all.at[pl.ds(1, n_band - 1)], row_recv.at[0])
        rows_all[0] = row[...]
        held = [rows_all[s] for s in range(n_band)]
        columns = []
        for m in range(SUB):
            total = held[0] * held[0][m : m + 1, :]
            for s in range(1, n_band):
                total = total + held[s] * held[s][m : m + 1, :]
            ident = jnp.where(lax.broadcasted_iota(jnp.int32, (SUB, LANES), 0) == m, RIDGE * n_band, 0.0)
            columns.append(total + ident.astype(f32))
        right = list(held)
        iota = lax.broadcasted_iota(jnp.int32, (SUB, LANES), 0)
        for i in range(SUB):
            inverse = 1.0 / columns[i][i : i + 1, :]
            factor = columns[i]
            for group in (columns, right):
                for c in range(len(group)):
                    lead = jnp.broadcast_to(group[c][i : i + 1, :] * inverse, (SUB, LANES))
                    group[c] = jnp.where(iota == i, lead, group[c] - factor * lead)

        def weight_of(a, b):
            return jnp.broadcast_to(jnp.sum(right[b] * held[a], axis=0, keepdims=True), (SUB, LANES))

        for s in range(n_band):
            band = from_of(s)
            gweights[band] = right[s]
            weights[band] = weight_of(0, s)
        if exchange:
            for a in range(n_band):
                for b in range(n_band):
                    wmat[a * n_band + b] = weight_of(a, b)

    x_copies = [{} for _ in range(ITERS)]
    ahead = n_band // 2
    behind = n_band - 1 - ahead

    def ring(turn):
        return 0 if exchange else turn

    def slot_of(way, distance):
        if distance > behind:
            return n_band - 1
        return distance + way * behind if distance else 0

    cuts = ring_cuts(exchange)
    units = dirs * cuts

    def reach_of(u, way):
        return ahead if way == u % 2 else behind

    order = [
        (u, way)
        for pair in zip(*[sorted(range(units), key=lambda u: -reach_of(u, way)) for way in range(2)])
        for way, u in enumerate(pair)
    ]

    def arrival(turn, u, way, distance):
        far = reach_of(u, way) == ahead
        if cuts == 1:
            return x_recv.at[ring(turn), u, slot_of(way, distance) - 1]
        if distance == reach_of(u, way):
            return x_far.at[2 * far + way]
        return x_recv.at[ring(turn), u, distance - 1 + (0 if far else ahead - 1)]

    def settle(turn, way, distance):
        half = way if distance == ahead else 1 - way
        rows = pl.ds(half * (8 // cuts), 8 // cuts)
        drain(
            xall.at[ring(turn), :, slot_of(way, distance), rows],
            x_far.at[2 * (distance == ahead) + way],
        )

    def send_x(turn, u, way, distance):
        to = slot_of(way, distance + 1)
        k, rows = u // cuts, pl.ds(u % cuts * (8 // cuts), 8 // cuts)
        copy = pltpu.make_async_remote_copy(
            src_ref=xall.at[ring(turn), k, slot_of(way, distance), rows],
            dst_ref=xall.at[ring(turn), k, to, rows],
            send_sem=x_send.at[0],
            recv_sem=arrival(turn, u, way, distance + 1),
            device_id={"band": nexts[way]},
            device_id_type=MESH,
        )
        copy.start()
        x_copies[turn][(u, way, distance + 1)] = copy

    def pump(turn, distance):
        for u, way in order:
            reach = reach_of(u, way)
            if distance < reach:
                x_copies[turn][(u, way, distance)].wait_recv()
                send_x(turn, u, way, distance)
            elif distance == reach and cuts == 1:
                x_copies[turn][(u, way, distance)].wait_recv()
        if cuts == 2 and distance in (behind, ahead):
            for way in range(2):
                settle(turn, way, distance)

    def source(slot):
        if slot <= behind:
            return at(lax.rem(pos + n_band - slot, n_band))
        return at(lax.rem(pos + slot - behind, n_band))

    def part_of(k, v):
        here = (v * dirs + k) * per
        return here // part_rows, pl.ds(here % part_rows, per)

    def send_parts(turn):
        for step in range(n_band - 1, 0, -1):
            pltpu.make_async_remote_copy(
                src_ref=xs.at[turn, to_of(step)],
                dst_ref=inbox.at[turn, own, step],
                send_sem=p_send.at[0],
                recv_sem=p_recv.at[turn, own],
                device_id={"band": to_of(step), "dir": leader},
                device_id_type=MESH,
            ).start()

        @pl.when(own == 0)
        def _():
            pltpu.make_async_remote_copy(
                src_ref=xs.at[turn, me],
                dst_ref=inbox.at[turn, 0, 0],
                send_sem=p_send.at[0],
                recv_sem=p_recv.at[turn, 0],
                device_id={"dir": flip(0)},
                device_id_type=MESH,
            ).start()

        @pl.when(own == 1)
        def _():
            inbox[turn, 1, 0] = xs[turn, me]

    def answer_parts(turn, side):
        if side == 0:
            drain(inbox.at[turn, 0], p_recv.at[turn, 0])
        else:
            drain(inbox.at[turn, 1, pl.ds(1, n_band - 1)], p_recv.at[turn, 1])
        for a in range(n_band - 1, -1, -1):
            for r in range(part_rows // SUB):
                here = slice(r * SUB, (r + 1) * SUB)
                total = wmat[a * n_band] * inbox[turn, side, 0, here, :]
                for b in range(1, n_band):
                    total = total + wmat[a * n_band + b] * inbox[turn, side, b, here, :]
                outbox[turn, side, a, here, :] = total
            if a or side == 0:
                pltpu.make_async_remote_copy(
                    src_ref=outbox.at[turn, side, a],
                    dst_ref=consin.at[turn, me],
                    send_sem=p_send.at[1],
                    recv_sem=p_recv.at[turn, 2],
                    device_id={"band": to_of(a), "dir": flip(0)} if side == 0 else {"band": to_of(a)},
                    device_id_type=MESH,
                ).start()

    def send_d(turn, n, c):
        if n == 0:
            src, dst = model.at[turn, c], got_a.at[turn, c]
        elif n < stages:
            src, dst = sums.at[turn, n - 1, c], got_b.at[turn, n - 1, c]
        else:
            src, dst = sums.at[turn, stages - 1, c], got_c.at[turn, c]
        return pltpu.make_async_remote_copy(
            src_ref=src,
            dst_ref=dst,
            send_sem=d_send.at[n],
            recv_sem=d_recv.at[0 if n % stages == 0 else 2 * n - 1 + turn % 2, c],
            device_id={"dir": flip(n if n < stages else 0)},
            device_id_type=MESH,
        )

    def end(comp, lane):
        return ends[comp * dirs : (comp + 1) * dirs, lane]

    def gram(a, b, lane):
        if a > b:
            return conj(gram(b, a, lane))
        n = pairs.index((a, b))
        real = grams[(2 * n) * dirs : (2 * n + 1) * dirs, lane]
        if a == b:
            return real
        return (real, grams[(2 * n + 1) * dirs : (2 * n + 2) * dirs, lane])

    def first_of(c):
        return slice(2 * c * LANES, (2 * c + 1) * LANES)

    def second_of(c):
        return slice((2 * c + 1) * LANES, (2 * c + 2) * LANES)

    def chunk_of(c):
        return slice(c * LANES, (c + 1) * LANES)

    for turn in range(ITERS):
        for g in range(nrow // SUB):
            for j in range(per):
                left = jones[pl.ds(g * SUB * per + j, SUB, stride=per), :]
                for piece in range(PIECES):
                    part = left.astype(jnp.bfloat16)
                    lhs[
                        piece * nrow + g * SUB : piece * nrow + (g + 1) * SUB,
                        j * LANES : (j + 1) * LANES,
                    ] = part
                    left = left - part.astype(f32)

        def gather(c, group):
            lane = slice(2 * c * LANES, 2 * (c + group) * LANES)
            ends[:, lane] = join(jnp.dot(lhs[...], gather_hot[:, lane], preferred_element_type=f32), nrow)

        def predict(c):
            lane, lane_p, lane_q = chunk_of(c), first_of(c), second_of(c)

            def model_body(h, carry):
                time = pl.ds(pl.multiple_of(h * SUB, SUB), SUB)
                total = [None] * 4
                for k in range(dirs):
                    co = [(coh[k, v, time, lane], coh[k, 4 + v, time, lane]) for v in range(4)]

                    def spread(v, where):
                        return tuple(
                            jnp.broadcast_to(
                                ends[(4 * part + v) * dirs + k : (4 * part + v) * dirs + k + 1, where],
                                (SUB, LANES),
                            )
                            for part in range(2)
                        )

                    p = [spread(v, lane_p) for v in range(4)]
                    q = [spread(v, lane_q) for v in range(4)]
                    for a in range(2):
                        b = [cadd(cmul(p[2 * a], co[d]), cmul(p[2 * a + 1], co[2 + d])) for d in range(2)]
                        for d in range(2):
                            term = cadd(cmul_conj(b[0], q[2 * d]), cmul_conj(b[1], q[2 * d + 1]))
                            v = 2 * a + d
                            total[v] = term if total[v] is None else cadd(total[v], term)
                for v in range(4):
                    model[turn, c, 0, v, time, :] = total[v][0]
                    model[turn, c, 1, v, time, :] = total[v][1]
                return carry

            lax.fori_loop(0, halves, model_body, 0)

        def collect(c):
            send_d(turn, 0, c).wait_recv()
            sums[turn, 0, c] = model[turn, c] + got_a[turn, c]
            if stages > 1:
                send_d(turn, 1, c).start()

        def collect_all(some):
            @pl.when(own == 1)
            def _():
                for c in some:
                    collect(c)

        begun = min(1, chunks - 1) if turn == 0 and chunks > 2 else 0
        for c in range(chunks):
            width = 1 if turn == 0 and c < group else group
            if c % width == 0:
                if turn == 0 and c > 0:
                    for e in range(width):
                        gather_setup(c + e)
                gather(c, width)
            if turn == 0 and c == 0:
                loads["coh"].wait()
            if begun and c == 2:
                collect_all(range(begun))
            predict(c)
            if turn == 0 and c == 0:
                first_sends()

            @pl.when(own == 0)
            def _():
                send_d(turn, 0, c).start()

        def collect_next(stage, c):
            send_d(turn, stage, c).wait_recv()
            sums[turn, stage, c] = sums[turn, stage - 1, c] + got_b[turn, stage - 1, c]
            if stage + 1 < stages:
                send_d(turn, stage + 1, c).start()

        def obtain(c):
            lane = chunk_of(c)

            @pl.when(own == 1)
            def _():
                if stages > 1:
                    collect_next(stages - 1, c)
                send_d(turn, stages, c).start()
                res[:, :, :, lane] = vis[:, :, :, lane] - sums[turn, stages - 1, c]

            @pl.when(own == 0)
            def _():
                send_d(turn, stages, c).wait_recv()
                res[:, :, :, lane] = vis[:, :, :, lane] - got_c[turn, c]

        def gram_of(j):
            m00 = re_mul(j[0], conj(j[0])) + re_mul(j[2], conj(j[2]))
            m11 = re_mul(j[1], conj(j[1])) + re_mul(j[3], conj(j[3]))
            m01 = cadd(cmul_conj(j[1], j[0]), cmul_conj(j[3], j[2]))
            return m00, m11, m01

        def ends_of(lane):
            return [(end(v, lane), end(4 + v, lane)) for v in range(4)]

        def normals(c):
            lane = chunk_of(c)

            def gr(a, b):
                return gram(a, b, lane)

            jp, jq = ends_of(first_of(c)), ends_of(second_of(c))
            m00, m11, m01 = gram_of(jq)
            p00, p11, p01 = gram_of(jp)
            n1_00 = m00 * gr(0, 0) + m11 * gr(1, 1) + 2.0 * re_mul(m01, gr(0, 1))
            n1_11 = m00 * gr(2, 2) + m11 * gr(3, 3) + 2.0 * re_mul(m01, gr(2, 3))
            n1_01 = cadd(
                cadd(scale(m00, gr(0, 2)), scale(m11, gr(1, 3))),
                cadd(cmul(m01, gr(0, 3)), cmul(conj(m01), gr(1, 2))),
            )
            n2_00 = p00 * gr(0, 0) + p11 * gr(2, 2) + 2.0 * re_mul(p01, gr(2, 0))
            n2_11 = p00 * gr(1, 1) + p11 * gr(3, 3) + 2.0 * re_mul(p01, gr(3, 1))
            n2_01 = cadd(
                cadd(scale(p00, gr(1, 0)), scale(p11, gr(3, 2))),
                cadd(cmul(p01, gr(3, 0)), cmul(conj(p01), gr(1, 2))),
            )
            for n, (left, right) in enumerate(
                ((n1_00, n2_00), (n1_11, n2_11), (n1_01[0], n2_01[0]), (n1_01[1], n2_01[1]))
            ):
                vals_n[n * dirs : (n + 1) * dirs, first_of(c)] = left
                vals_n[n * dirs : (n + 1) * dirs, second_of(c)] = right

        def scatter_normals():
            split_store(lhs_n, 4 * dirs, vals_n[...])
            out = join(jnp.dot(lhs_n[...], scatter_hot[...], preferred_element_type=f32), 4 * dirs)
            for g in range(4 * dirs // SUB):
                for j in range(per):
                    seg_n[pl.ds(g * SUB * per + j, SUB, stride=per), :] = out[
                        g * SUB : (g + 1) * SUB, j * LANES : (j + 1) * LANES
                    ]

        def finish(c):
            lane = chunk_of(c)
            r = [[res[v // 4, v % 4, h * SUB : (h + 1) * SUB, lane] for h in range(halves)] for v in range(8)]
            for k in range(dirs):
                co = [[coh[k, v, h * SUB : (h + 1) * SUB, lane] for h in range(halves)] for v in range(8)]
                for a in range(4):
                    for b in range(4):
                        real = sum(r[a][h] * co[b][h] + r[4 + a][h] * co[4 + b][h] for h in range(halves))
                        imag = sum(r[4 + a][h] * co[b][h] - r[a][h] * co[4 + b][h] for h in range(halves))
                        n = 2 * (4 * a + b)
                        cross[n * dirs + k : n * dirs + k + 1, lane] = jnp.sum(real, axis=0, keepdims=True)
                        cross[(n + 1) * dirs + k : (n + 1) * dirs + k + 1, lane] = jnp.sum(
                            imag, axis=0, keepdims=True
                        )

            def crossed(a, b):
                n = 2 * (4 * a + b)
                return (
                    cross[n * dirs : (n + 1) * dirs, lane],
                    cross[(n + 1) * dirs : (n + 2) * dirs, lane],
                )

            jp, jq = ends_of(first_of(c)), ends_of(second_of(c))
            for which, j, other_end in ((0, jq, jp), (1, jp, jq)):
                where = second_of(c) if which else first_of(c)
                h00, h11, re01, im01 = [vals_n[n * dirs : (n + 1) * dirs, where] for n in range(4)]
                h01 = (re01, im01)
                for a in range(2):
                    for d in range(2):
                        total = None
                        for b in range(2):
                            for e in range(2):
                                if which == 0:
                                    term = cmul(j[2 * b + e], crossed(2 * a + b, 2 * d + e))
                                else:
                                    term = cmul_conj(j[2 * b + e], crossed(2 * b + a, 2 * e + d))
                                total = term if total is None else cadd(total, term)
                        if d == 0:
                            extra = cadd(scale(h00, other_end[2 * a]), cmul_conj(other_end[2 * a + 1], h01))
                        else:
                            extra = cadd(cmul(other_end[2 * a], h01), scale(h11, other_end[2 * a + 1]))
                        total = cadd(total, extra)
                        for part in range(2):
                            n = 4 * part + 2 * a + d
                            vals[n * dirs : (n + 1) * dirs, which * LANES : (which + 1) * LANES] = total[part]

            split_store(lhs_c, nrow, vals[...])
            rows = slice(2 * c * LANES, (2 * c + 2) * LANES)
            out = join(jnp.dot(lhs_c[...], scatter_hot[rows, :], preferred_element_type=f32), nrow)
            if c > 0:
                out = out + found[...]
            if c + 1 < chunks:
                found[...] = out
            else:
                for g in range(nrow // SUB):
                    for j in range(per):
                        seg[pl.ds(g * SUB * per + j, SUB, stride=per), :] = out[
                            g * SUB : (g + 1) * SUB, j * LANES : (j + 1) * LANES
                        ]

        if turn == 0:
            collect_all(range(begun, begun + 1))
            lax.fori_loop(0, chunks, gram_body, 0)
        for c in range(chunks):
            normals(c)
        if turn == 0:
            hear(0)
        else:
            scatter_normals()
        collect_all(range(begun + 1 if turn == 0 else 0, chunks))
        if turn == 0:
            scatter_setup()
            start_consensus()
            hear(1)
            loads["vis"].wait()
        if turn > 0 and exchange:

            @pl.when(own == 1)
            def _():
                if turn == 1:
                    solve_weights()
                answer_parts(turn - 1, 1)

            if turn == 2:

                @pl.when(own == 0)
                def _():
                    solve_weights()

        if turn == 1 and not exchange:
            solve_weights()
        if stages > 2:

            @pl.when(own == 1)
            def _():
                for stage in range(1, stages - 1):
                    for c in range(chunks):
                        collect_next(stage, c)

        for c in range(chunks):
            obtain(c)
            if turn > 0 and exchange and c == ANSWER:

                @pl.when(own == 1)
                def _():
                    answer_parts(turn - 1, 0)

            if turn == 0 and c == min(1, chunks - 1):
                scatter_normals()
            finish(c)
            if turn == 0 and c == min(1, chunks - 1):
                for r in range(2, max(2, rounds)):
                    hear(r)
                send_rows()

        def refresh(k, v, total, previous):
            here = packed(k, v)
            fresh = dual[here, :] + RHO * (jones[here, :] - total)
            if previous + 1 < ITERS:
                cons[here, :] = total
                dual[here, :] = fresh
            else:
                dual_out[halves_of(k, v)] = fresh

        def join_parts(previous):
            @pl.when(own == 0)
            def _():
                drain(consin.at[previous], p_recv.at[previous, 2])

            @pl.when(own == 1)
            def _():
                drain(consin.at[previous, pl.ds(1, n_band - 1)], p_recv.at[previous, 2])
                consin[previous, me] = outbox[previous, 1, 0]

            for k in range(dirs):
                for v in range(8):
                    part, rows = part_of(k, v)
                    refresh(k, v, consin[previous, part, rows, :], previous)

        def ring_sum(turn, k, v, slots, total=None):
            for s in slots:
                term = weights[source(s)] * xall[ring(turn), k, s, v]
                total = term if total is None else total + term
            return total

        if turn > 0:
            if exchange:
                join_parts(turn - 1)
            else:
                for s in range(1, ahead + 1):
                    pump(turn - 1, s)
                for k in range(dirs):
                    for v in range(8):
                        refresh(k, v, ring_sum(turn - 1, k, v, range(n_band)), turn - 1)

        by_ring = turn + 1 == ITERS or not exchange
        for k in range(dirs):
            y = []
            for v in range(8):
                here = packed(k, v)
                y.append(seg[here, :] + RHO * cons[here, :] - dual[here, :])
            h00, h11, re01, im01 = [seg_n[packed(k, n), :] for n in range(4)]
            h00 = h00 + RHO
            h11 = h11 + RHO
            inverse = 1.0 / (h00 * h11 - (re01 * re01 + im01 * im01))
            h00, h11, h01 = h00 * inverse, h11 * inverse, (re01 * inverse, im01 * inverse)
            for a in range(2):
                y0, y1 = (y[2 * a], y[4 + 2 * a]), (y[2 * a + 1], y[4 + 2 * a + 1])
                minus0, minus1 = cmul_conj(y1, h01), cmul(y0, h01)
                for part in range(2):
                    for c in range(2):
                        if c == 0:
                            value = h11 * y0[part] - minus0[part]
                        else:
                            value = h00 * y1[part] - minus1[part]
                        v = 4 * part + 2 * a + c
                        here = packed(k, v)
                        jones[here, :] = value
                        if turn + 1 == ITERS:
                            jones_out[halves_of(k, v)] = value
                        sent = value + dual[here, :] * (1.0 / RHO)
                        if by_ring:
                            xall[ring(turn), k, 0, v] = sent
                        else:
                            chunk, rows = part_of(k, v)
                            xs[turn, chunk, rows, :] = sent
        if by_ring:
            for u, way in order:
                if reach_of(u, way):
                    send_x(turn, u, way, 0)
        else:
            send_parts(turn)

    last = ITERS - 1
    for s in range(1, ahead):
        pump(last, s)

    def coeff_body(slots, first):
        def run(m, carry):
            for k in range(dirs):
                total = [None] * 8 if first else [coeffs[(m,) + halves_of(k, v)] for v in range(8)]
                for s in slots:
                    factor = jnp.broadcast_to(gweights[source(s), pl.ds(m, 1), :], (SUB, LANES))
                    for v in range(8):
                        term = factor * xall[ring(last), k, s, v]
                        total[v] = term if total[v] is None else total[v] + term
                for v in range(8):
                    coeffs[(m,) + halves_of(k, v)] = total[v]
            return carry

        lax.fori_loop(0, SUB, run, 0)

    early = range(n_band - 1)
    coeff_body(early, True)
    for k in range(dirs):
        for v in range(8):
            cons[packed(k, v), :] = ring_sum(last, k, v, early)
    pump(last, ahead)
    late = range(n_band - 1, n_band)
    for k in range(dirs):
        for v in range(8):
            refresh(k, v, ring_sum(last, k, v, late, cons[packed(k, v), :]), last)
    coeff_body(late, False)

    drain(rows_all.at[pl.ds(1, n_band - 1)], row_send.at[0])
    drain(xall.at[:, :, pl.ds(1, n_band - 1)], x_send.at[0])

    @pl.when(own == 0)
    def _():
        drain(model, d_send.at[0])
        if exchange:
            drain(xs, p_send.at[0])

    @pl.when(own == 1)
    def _():
        for n in range(1, stages + 1):
            drain(model, d_send.at[n])
        if exchange:
            drain(inbox.at[:, 1, pl.ds(1, n_band - 1)], p_send.at[0])
            drain(inbox.at[:, 0], p_send.at[1])
            drain(inbox.at[:, 1, pl.ds(1, n_band - 1)], p_send.at[1])


def flush(*refs):
    count = (len(refs) - 1) // 2
    sem = refs[-1]
    copies = [pltpu.make_async_copy(refs[n], refs[count + n], sem.at[n]) for n in range(count)]
    for copy in copies:
        copy.start()
    for copy in copies:
        copy.wait()


def power_of_two(n):
    return n & (n - 1) == 0


def ring_cuts(exchange):
    return 2 if exchange else 1


def by_chunks(n_band, rows):
    return power_of_two(n_band) and rows % (n_band * SUB) == 0


def local(n_band, n_dir, vis, coh, jones_start, dual_start, consensus_start, freq_basis, pairs):
    f32 = jnp.float32
    dirs, times, base = coh.shape[1], coh.shape[-2], coh.shape[-1]
    stations = jones_start.shape[-1]
    per = stations // LANES
    nrow = 8 * dirs
    terms = freq_basis.shape[1]

    def enter(value):
        lead = value.shape[:-2]
        value = value.reshape(lead + (2, per, LANES))
        return jnp.swapaxes(value, -2, -3).reshape(lead + (2 * per, LANES))

    def leave(value, shape):
        value = value.reshape(value.shape[:-2] + (per, 2, LANES))
        return jnp.swapaxes(value, -2, -3).reshape(shape)

    stages = n_dir.bit_length() - 1
    chunks = base // LANES
    exchange = by_chunks(n_band, nrow * per)
    rings = 1 if exchange else ITERS
    parts = (ITERS - 1, n_band, max(SUB, nrow * per // n_band), LANES) if exchange else (1, 1, SUB, LANES)
    half = (4, times, base)
    piece = (2, 4, times, LANES)
    vmem = pl.BlockSpec(memory_space=pltpu.VMEM)
    far = pl.BlockSpec(memory_space=pltpu.HBM)
    raw = (dirs, 4, 2 * per, LANES)
    raw_out = jax.ShapeDtypeStruct(raw, f32)
    raw_terms = jax.ShapeDtypeStruct((terms,) + raw, f32)
    bf16 = jnp.bfloat16
    operands = (
        vis.reshape((2,) + half),
        coh.reshape(dirs, 8, times, base),
        enter(jones_start.reshape((dirs, 4, 2, stations))),
        enter(dual_start.reshape((dirs, 4, 2, stations))),
        enter(consensus_start.reshape((terms, dirs, 4, 2, stations))),
        freq_basis,
        pairs,
    )
    results = pl.pallas_call(
        functools.partial(kernel, n_band, n_dir, dirs, times, base, stations),
        out_shape=(pltpu.VMEM(raw, f32), pltpu.VMEM(raw, f32), pltpu.VMEM((terms,) + raw, f32)),
        in_specs=[far] * 7,
        out_specs=(vmem,) * 3,
        scratch_shapes=[
            pltpu.VMEM((2,) + half, f32),
            pltpu.VMEM((dirs, 8, times, base), f32),
            pltpu.VMEM(raw, f32),
            pltpu.VMEM(raw, f32),
            pltpu.VMEM((terms,) + raw, f32),
            pltpu.SMEM(freq_basis.shape, f32),
            pltpu.VMEM((2, base), jnp.int32),
            pltpu.VMEM((nrow * per, LANES), f32),
            pltpu.VMEM((nrow * per, LANES), f32),
            pltpu.VMEM((SUB, LANES), f32),
            pltpu.VMEM((2 * base, LANES), jnp.int32),
            pltpu.VMEM((nrow * per, LANES), f32),
            pltpu.VMEM((rings, dirs, n_band, 8, per, LANES), f32),
            pltpu.VMEM((n_band, SUB, LANES), f32),
            pltpu.VMEM((n_band, SUB, LANES), f32),
            pltpu.VMEM((n_band, SUB, LANES), f32),
            pltpu.VMEM((n_band * n_band if exchange else 1, SUB, LANES), f32),
            pltpu.VMEM(parts, f32),
            pltpu.VMEM(parts[:1] + (2,) + parts[1:], f32),
            pltpu.VMEM(parts[:1] + (2,) + parts[1:], f32),
            pltpu.VMEM(parts, f32),
            pltpu.VMEM((stations, 2 * base), bf16),
            pltpu.VMEM((2 * base, stations), bf16),
            pltpu.VMEM((PIECES * nrow, stations), bf16),
            pltpu.VMEM((PIECES * nrow, 2 * LANES), bf16),
            pltpu.VMEM((PIECES * 4 * dirs, 2 * base), bf16),
            pltpu.VMEM((nrow, 2 * base), f32),
            pltpu.VMEM((20 * dirs, base), f32),
            pltpu.VMEM((32 * dirs, base), f32),
            pltpu.VMEM((nrow, 2 * LANES), f32),
            pltpu.VMEM((4 * dirs, 2 * base), f32),
            pltpu.VMEM((nrow, stations), f32),
            pltpu.VMEM((nrow * per, LANES), f32),
            pltpu.VMEM((4 * dirs * per, LANES), f32),
            pltpu.VMEM((ITERS, chunks) + piece, f32),
            pltpu.VMEM((ITERS, chunks) + piece, f32),
            pltpu.VMEM((ITERS, stages, chunks) + piece, f32),
            pltpu.VMEM((ITERS, max(1, stages - 1), chunks) + piece, f32),
            pltpu.VMEM((ITERS, chunks) + piece, f32),
            pltpu.VMEM((2,) + half, f32),
            pltpu.SemaphoreType.REGULAR((max(1, n_band // 2 - 1) if exchange else 1,)),
            pltpu.SemaphoreType.DMA((7,)),
            pltpu.SemaphoreType.DMA((1,)),
            pltpu.SemaphoreType.DMA((1,)),
            pltpu.SemaphoreType.DMA((2,)),
            pltpu.SemaphoreType.DMA((ITERS - 1, 3)),
            pltpu.SemaphoreType.DMA((1,)),
            pltpu.SemaphoreType.DMA((rings, dirs * ring_cuts(exchange), max(1, n_band - 3) if exchange else n_band - 1)),
            pltpu.SemaphoreType.DMA((4,)),
            pltpu.SemaphoreType.DMA((stages + 1,)),
            pltpu.SemaphoreType.DMA((2 * stages - 1, chunks)),
        ],
        compiler_params=pltpu.CompilerParams(
            collective_id=0, has_side_effects=True, vmem_limit_bytes=56 * 1024 * 1024
        ),
    )(*[pltpu.with_memory_space_constraint(x, pltpu.HBM) for x in operands])
    jones, dual, coeffs = pl.pallas_call(
        flush,
        out_shape=(raw_out, raw_out, raw_terms),
        in_specs=[vmem] * 3,
        out_specs=(pl.BlockSpec(memory_space=pltpu.HBM),) * 3,
        scratch_shapes=[pltpu.SemaphoreType.DMA((3,))],
        compiler_params=pltpu.CompilerParams(vmem_limit_bytes=1024 * 1024),
    )(*[pltpu.with_memory_space_constraint(x, pltpu.VMEM) for x in results])
    return (
        leave(jones, jones_start.shape),
        leave(dual, jones_start.shape),
        leave(coeffs, consensus_start.shape),
    )


def solution(mesh):
    in_specs = (
        P("band", None, None, None, None, None),
        P("band", "dir", None, None, None, None, None),
        P("band", "dir", None, None, None, None),
        P("band", "dir", None, None, None, None),
        P(None, "dir", None, None, None, None),
        P("band", None),
        P(),
    )
    out_specs = (
        P("band", "dir", None, None, None, None),
        P("band", "dir", None, None, None, None),
        P(None, "dir", None, None, None, None),
    )
    body = functools.partial(local, mesh.shape["band"], mesh.shape["dir"])
    return jax.shard_map(body, mesh=mesh, in_specs=in_specs, out_specs=out_specs, check_vma=False)
```

```python
import functools

import jax
import jax.numpy as jnp
from jax import lax
from jax.experimental import pallas as pl
from jax.experimental.pallas import tpu as pltpu
from jax.sharding import PartitionSpec as P

ITERS = 3
RHO = 5.0
RIDGE = 0.25
LANES = 128
SUB = 8
PIECES = 3
ANSWER = 0
MESH = pl.DeviceIdType.MESH


def cmul(a, b):
    return (a[0] * b[0] - a[1] * b[1], a[0] * b[1] + a[1] * b[0])


def cmul_conj(a, b):
    return (a[0] * b[0] + a[1] * b[1], a[1] * b[0] - a[0] * b[1])


def cadd(a, b):
    return (a[0] + b[0], a[1] + b[1])


def conj(a):
    return (a[0], -a[1])


def re_mul(a, b):
    return a[0] * b[0] - a[1] * b[1]


def scale(r, a):
    return (r * a[0], r * a[1])


def split_store(ref, rows, value):
    left = value
    for piece in range(PIECES):
        part = left.astype(jnp.bfloat16)
        ref[piece * rows : (piece + 1) * rows, :] = part
        if piece + 1 < PIECES:
            left = left - part.astype(jnp.float32)


def join(value, rows):
    total = value[0:rows]
    for piece in range(1, PIECES):
        total = total + value[piece * rows : (piece + 1) * rows]
    return total


def kernel(
    n_band, n_dir, dirs, times, base, stations,
    vis_far, coh_far, jones0_far, dual0_far, coeffs0_far, basis_far, pairs_far,
    jones_out, dual_out, coeffs,
    vis, coh, jones0, dual0, coeffs0, basis, pairs_ref,
    jones, dual, row, ids_col,
    cons, xall, rows_all, weights, gweights, wmat,
    xs, inbox, outbox, consin,
    gather_hot, scatter_hot, lhs, lhs_c, lhs_n, ends, grams, cross, vals, vals_n, found, seg, seg_n,
    model, got_a, sums, got_b, got_c, res,
    greet_sem, load_sem, row_send, row_recv, p_send, p_recv, x_send, x_recv, x_far, d_send, d_recv,
):
    f32 = jnp.float32
    nrow = 8 * dirs
    per = stations // LANES
    me = lax.axis_index("band")
    mine = lax.axis_index("dir")
    chunks = base // LANES
    halves = times // SUB
    stages = n_dir.bit_length() - 1
    part_rows = nrow * per // n_band
    exchange = by_chunks(n_band, nrow * per)

    def at(pos):
        half = pos // (n_band // 2)
        return (1 - half) * (2 * pos) + half * (2 * (n_band - 1 - pos) + 1)

    odd = lax.rem(me, 2)
    pos = (1 - odd) * (me // 2) + odd * (n_band - 1 - me // 2)
    nexts = (at(lax.rem(pos + 1, n_band)), at(lax.rem(pos + n_band - 1, n_band)))

    def flip_bits(index, mask):
        out = index
        for b in range(mask.bit_length()):
            if mask >> b & 1:
                out = out + (1 - 2 * lax.rem(index // (1 << b), 2)) * (1 << b)
        return out

    def to_of(step):
        return flip_bits(me, step) if power_of_two(n_band) else lax.rem(me + step, n_band)

    def from_of(step):
        return flip_bits(me, step) if power_of_two(n_band) else lax.rem(me + n_band - step, n_band)

    def flip(stage):
        return flip_bits(mine, 1 << stage)

    def drain(ref, sem):
        pltpu.make_async_copy(ref, ref, sem).wait()

    own = lax.rem(mine, 2)
    leader = mine + 1 - own

    def columns_of(c):
        return (slice(None), slice(None), slice(None), pl.ds(c * LANES, LANES))

    cuts_of = [(c, coh_far.at[columns_of(c)], coh.at[columns_of(c)]) for c in range(chunks)]
    urgent = [("pairs", pairs_far, pairs_ref), ("jones", jones0_far, jones0), cuts_of[0]]
    patient = cuts_of[1:] + [
        ("basis", basis_far, basis),
        ("vis", vis_far, vis),
        ("dual", dual0_far, dual0),
        ("coeffs", coeffs0_far, coeffs0),
    ]
    loads = {}

    def load(some):
        for name, source_ref, near in some:
            loads[name] = pltpu.make_async_copy(source_ref, near, load_sem.at[len(loads)])
            loads[name].start()

    load(urgent)

    ways = min(2, n_band - 1)
    rounds = n_band // 2 - 1 if exchange else 0
    band_peers = list(nexts[:ways]) if exchange else [to_of(step) for step in range(1, n_band)]
    barrier = pltpu.get_barrier_semaphore()
    for peer in band_peers:
        pl.semaphore_signal(barrier, inc=1, device_id={"band": peer}, device_id_type=MESH)
    for stage in range(stages):
        pl.semaphore_signal(barrier, inc=1, device_id={"dir": flip(stage)}, device_id_type=MESH)

    def greet(r):
        if r < rounds:
            for way in range(ways):
                pl.semaphore_signal(
                    greet_sem.at[r], inc=1, device_id={"band": nexts[way]}, device_id_type=MESH
                )

    def hear(r):
        if r < rounds:
            pl.semaphore_wait(greet_sem.at[r], ways)
            greet(r + 1)

    def halves_of(k, v):
        return (k, v // 2, pl.ds(v % 2, per, stride=2), slice(None))

    def packed(k, v):
        return pl.ds((v * dirs + k) * per, per)

    def block_of(j):
        return j % 2, (j // 2) * LANES

    def gather_setup(c):
        step_rows = LANES

        def hot_body(i, carry):
            start = pl.multiple_of(i * step_rows, step_rows)
            sid = lax.broadcasted_iota(jnp.int32, (step_rows, LANES), 0) + i * step_rows
            for j in (2 * c, 2 * c + 1):
                lane = slice(j * LANES, (j + 1) * LANES)
                which, low = block_of(j)
                ids = pairs_ref[which : which + 1, low : low + LANES]
                same = sid == jnp.broadcast_to(ids, (step_rows, LANES))
                gather_hot[pl.ds(start, step_rows), lane] = jnp.where(same, 1.0, 0.0).astype(jnp.bfloat16)
            return carry

        lax.fori_loop(0, stations // step_rows, hot_body, 0)

    loads["pairs"].wait()
    load(patient)
    group = 2 - chunks % 2
    gather_setup(0)
    loads["jones"].wait()
    for k in range(dirs):
        for v in range(8):
            jones[packed(k, v), :] = jones0[halves_of(k, v)]

    def scatter_setup():
        step_rows = 32

        for j in range(2 * chunks):
            which, low = block_of(j)
            ids = jnp.broadcast_to(pairs_ref[which : which + 1, low : low + LANES], (LANES, LANES))
            ids_col[j * LANES : (j + 1) * LANES, :] = jnp.transpose(ids)

        def hot_body2(i, carry):
            start = pl.multiple_of(i * step_rows, step_rows)
            col = ids_col[pl.ds(start, step_rows), :]
            for j in range(stations // LANES):
                lane = slice(j * LANES, (j + 1) * LANES)
                sid = lax.broadcasted_iota(jnp.int32, (step_rows, LANES), 1) + j * LANES
                scatter_hot[pl.ds(start, step_rows), lane] = jnp.where(sid == col, 1.0, 0.0).astype(jnp.bfloat16)
            return carry

        lax.fori_loop(0, 2 * base // step_rows, hot_body2, 0)

    def first_sends():
        pl.semaphore_wait(barrier, len(band_peers) + stages)
        greet(0)
        loads["basis"].wait()
        row[...] = jnp.zeros((SUB, LANES), f32)
        for m in range(SUB):
            row[m : m + 1, :] = jnp.full((1, LANES), basis[0, m], f32)

    def send_rows():
        for step in range(1, n_band):
            pltpu.make_async_remote_copy(
                src_ref=row,
                dst_ref=rows_all.at[step],
                send_sem=row_send.at[0],
                recv_sem=row_recv.at[0],
                device_id={"band": to_of(step)},
                device_id_type=MESH,
            ).start()

    pairs = [(a, b) for a in range(4) for b in range(a, 4)]

    def gram_body(j, carry):
        lane = pl.ds(pl.multiple_of(j * LANES, LANES), LANES)
        for k in range(dirs):
            c = [
                [coh[k, v, h * SUB : (h + 1) * SUB, lane] for h in range(halves)]
                for v in range(8)
            ]
            for n, (a, b) in enumerate(pairs):
                real = sum(c[a][h] * c[b][h] + c[4 + a][h] * c[4 + b][h] for h in range(halves))
                grams[(2 * n) * dirs + k : (2 * n) * dirs + k + 1, lane] = jnp.sum(real, axis=0, keepdims=True)
                if a != b:
                    imag = sum(c[4 + a][h] * c[b][h] - c[a][h] * c[4 + b][h] for h in range(halves))
                    grams[(2 * n + 1) * dirs + k : (2 * n + 1) * dirs + k + 1, lane] = jnp.sum(
                        imag, axis=0, keepdims=True
                    )
        return carry

    def start_consensus():
        loads["coeffs"].wait()
        loads["dual"].wait()
        for k in range(dirs):
            for v in range(8):
                dual[packed(k, v), :] = dual0[halves_of(k, v)]
                total = basis[0, 0] * coeffs0[(0,) + halves_of(k, v)]
                for m in range(1, SUB):
                    total = total + basis[0, m] * coeffs0[(m,) + halves_of(k, v)]
                cons[packed(k, v), :] = total

    def solve_weights():
        drain(rows_all.at[pl.ds(1, n_band - 1)], row_recv.at[0])
        rows_all[0] = row[...]
        held = [rows_all[s] for s in range(n_band)]
        columns = []
        for m in range(SUB):
            total = held[0] * held[0][m : m + 1, :]
            for s in range(1, n_band):
                total = total + held[s] * held[s][m : m + 1, :]
            ident = jnp.where(lax.broadcasted_iota(jnp.int32, (SUB, LANES), 0) == m, RIDGE * n_band, 0.0)
            columns.append(total + ident.astype(f32))
        right = list(held)
        iota = lax.broadcasted_iota(jnp.int32, (SUB, LANES), 0)
        for i in range(SUB):
            inverse = 1.0 / columns[i][i : i + 1, :]
            factor = columns[i]
            for group in (columns, right):
                for c in range(len(group)):
                    lead = jnp.broadcast_to(group[c][i : i + 1, :] * inverse, (SUB, LANES))
                    group[c] = jnp.where(iota == i, lead, group[c] - factor * lead)

        def weight_of(a, b):
            return jnp.broadcast_to(jnp.sum(right[b] * held[a], axis=0, keepdims=True), (SUB, LANES))

        for s in range(n_band):
            band = from_of(s)
            gweights[band] = right[s]
            weights[band] = weight_of(0, s)
        if exchange:
            for a in range(n_band):
                for b in range(n_band):
                    wmat[a * n_band + b] = weight_of(a, b)

    x_copies = [{} for _ in range(ITERS)]
    ahead = n_band // 2
    behind = n_band - 1 - ahead

    def ring(turn):
        return 0 if exchange else turn

    def slot_of(way, distance):
        if distance > behind:
            return n_band - 1
        return distance + way * behind if distance else 0

    cuts = ring_cuts(exchange)
    units = dirs * cuts

    def reach_of(u, way):
        return ahead if way == u % 2 else behind

    order = [
        (u, way)
        for pair in zip(*[sorted(range(units), key=lambda u: -reach_of(u, way)) for way in range(2)])
        for way, u in enumerate(pair)
    ]

    def arrival(turn, u, way, distance):
        far = reach_of(u, way) == ahead
        if cuts == 1:
            return x_recv.at[ring(turn), u, slot_of(way, distance) - 1]
        if distance == reach_of(u, way):
            return x_far.at[2 * far + way]
        return x_recv.at[ring(turn), u, distance - 1 + (0 if far else ahead - 1)]

    def settle(turn, way, distance):
        half = way if distance == ahead else 1 - way
        rows = pl.ds(half * (8 // cuts), 8 // cuts)
        drain(
            xall.at[ring(turn), :, slot_of(way, distance), rows],
            x_far.at[2 * (distance == ahead) + way],
        )

    def send_x(turn, u, way, distance):
        to = slot_of(way, distance + 1)
        k, rows = u // cuts, pl.ds(u % cuts * (8 // cuts), 8 // cuts)
        copy = pltpu.make_async_remote_copy(
            src_ref=xall.at[ring(turn), k, slot_of(way, distance), rows],
            dst_ref=xall.at[ring(turn), k, to, rows],
            send_sem=x_send.at[0],
            recv_sem=arrival(turn, u, way, distance + 1),
            device_id={"band": nexts[way]},
            device_id_type=MESH,
        )
        copy.start()
        x_copies[turn][(u, way, distance + 1)] = copy

    def pump(turn, distance):
        for u, way in order:
            reach = reach_of(u, way)
            if distance < reach:
                x_copies[turn][(u, way, distance)].wait_recv()
                send_x(turn, u, way, distance)
            elif distance == reach and cuts == 1:
                x_copies[turn][(u, way, distance)].wait_recv()
        if cuts == 2 and distance in (behind, ahead):
            for way in range(2):
                settle(turn, way, distance)

    def source(slot):
        if slot <= behind:
            return at(lax.rem(pos + n_band - slot, n_band))
        return at(lax.rem(pos + slot - behind, n_band))

    def part_of(k, v):
        here = (v * dirs + k) * per
        return here // part_rows, pl.ds(here % part_rows, per)

    def send_parts(turn):
        for step in range(n_band - 1, 0, -1):
            pltpu.make_async_remote_copy(
                src_ref=xs.at[turn, to_of(step)],
                dst_ref=inbox.at[turn, own, step],
                send_sem=p_send.at[0],
                recv_sem=p_recv.at[turn, own],
                device_id={"band": to_of(step), "dir": leader},
                device_id_type=MESH,
            ).start()

        @pl.when(own == 0)
        def _():
            pltpu.make_async_remote_copy(
                src_ref=xs.at[turn, me],
                dst_ref=inbox.at[turn, 0, 0],
                send_sem=p_send.at[0],
                recv_sem=p_recv.at[turn, 0],
                device_id={"dir": flip(0)},
                device_id_type=MESH,
            ).start()

        @pl.when(own == 1)
        def _():
            inbox[turn, 1, 0] = xs[turn, me]

    def answer_parts(turn, side):
        if side == 0:
            drain(inbox.at[turn, 0], p_recv.at[turn, 0])
        else:
            drain(inbox.at[turn, 1, pl.ds(1, n_band - 1)], p_recv.at[turn, 1])
        for a in range(n_band - 1, -1, -1):
            for r in range(part_rows // SUB):
                here = slice(r * SUB, (r + 1) * SUB)
                total = wmat[a * n_band] * inbox[turn, side, 0, here, :]
                for b in range(1, n_band):
                    total = total + wmat[a * n_band + b] * inbox[turn, side, b, here, :]
                outbox[turn, side, a, here, :] = total
            if a or side == 0:
                pltpu.make_async_remote_copy(
                    src_ref=outbox.at[turn, side, a],
                    dst_ref=consin.at[turn, me],
                    send_sem=p_send.at[1],
                    recv_sem=p_recv.at[turn, 2],
                    device_id={"band": to_of(a), "dir": flip(0)} if side == 0 else {"band": to_of(a)},
                    device_id_type=MESH,
                ).start()

    def send_d(turn, n, c):
        if n == 0:
            src, dst = model.at[turn, c], got_a.at[turn, c]
        elif n < stages:
            src, dst = sums.at[turn, n - 1, c], got_b.at[turn, n - 1, c]
        else:
            src, dst = sums.at[turn, stages - 1, c], got_c.at[turn, c]
        return pltpu.make_async_remote_copy(
            src_ref=src,
            dst_ref=dst,
            send_sem=d_send.at[n],
            recv_sem=d_recv.at[0 if n % stages == 0 else 2 * n - 1 + turn % 2, c],
            device_id={"dir": flip(n if n < stages else 0)},
            device_id_type=MESH,
        )

    def end(comp, lane):
        return ends[comp * dirs : (comp + 1) * dirs, lane]

    def gram(a, b, lane):
        if a > b:
            return conj(gram(b, a, lane))
        n = pairs.index((a, b))
        real = grams[(2 * n) * dirs : (2 * n + 1) * dirs, lane]
        if a == b:
            return real
        return (real, grams[(2 * n + 1) * dirs : (2 * n + 2) * dirs, lane])

    def first_of(c):
        return slice(2 * c * LANES, (2 * c + 1) * LANES)

    def second_of(c):
        return slice((2 * c + 1) * LANES, (2 * c + 2) * LANES)

    def chunk_of(c):
        return slice(c * LANES, (c + 1) * LANES)

    for turn in range(ITERS):
        for g in range(nrow // SUB):
            for j in range(per):
                left = jones[pl.ds(g * SUB * per + j, SUB, stride=per), :]
                for piece in range(PIECES):
                    part = left.astype(jnp.bfloat16)
                    lhs[
                        piece * nrow + g * SUB : piece * nrow + (g + 1) * SUB,
                        j * LANES : (j + 1) * LANES,
                    ] = part
                    left = left - part.astype(f32)

        def gather(c, group):
            lane = slice(2 * c * LANES, 2 * (c + group) * LANES)
            ends[:, lane] = join(jnp.dot(lhs[...], gather_hot[:, lane], preferred_element_type=f32), nrow)

        def predict(c):
            lane, lane_p, lane_q = chunk_of(c), first_of(c), second_of(c)

            def model_body(h, carry):
                time = pl.ds(pl.multiple_of(h * SUB, SUB), SUB)
                total = [None] * 4
                for k in range(dirs):
                    co = [(coh[k, v, time, lane], coh[k, 4 + v, time, lane]) for v in range(4)]

                    def spread(v, where):
                        return tuple(
                            jnp.broadcast_to(
                                ends[(4 * part + v) * dirs + k : (4 * part + v) * dirs + k + 1, where],
                                (SUB, LANES),
                            )
                            for part in range(2)
                        )

                    p = [spread(v, lane_p) for v in range(4)]
                    q = [spread(v, lane_q) for v in range(4)]
                    for a in range(2):
                        b = [cadd(cmul(p[2 * a], co[d]), cmul(p[2 * a + 1], co[2 + d])) for d in range(2)]
                        for d in range(2):
                            term = cadd(cmul_conj(b[0], q[2 * d]), cmul_conj(b[1], q[2 * d + 1]))
                            v = 2 * a + d
                            total[v] = term if total[v] is None else cadd(total[v], term)
                for v in range(4):
                    model[turn, c, 0, v, time, :] = total[v][0]
                    model[turn, c, 1, v, time, :] = total[v][1]
                return carry

            lax.fori_loop(0, halves, model_body, 0)

        def collect(c):
            send_d(turn, 0, c).wait_recv()
            sums[turn, 0, c] = model[turn, c] + got_a[turn, c]
            if stages > 1:
                send_d(turn, 1, c).start()

        def collect_all(some):
            @pl.when(own == 1)
            def _():
                for c in some:
                    collect(c)

        begun = min(1, chunks - 1) if turn == 0 and chunks > 2 else 0
        for c in range(chunks):
            width = 1 if turn == 0 and c < group else group
            if c % width == 0:
                if turn == 0 and c > 0:
                    for e in range(width):
                        gather_setup(c + e)
                gather(c, width)
            if turn == 0:
                loads[c].wait()
            if begun and c == 2:
                collect_all(range(begun))
            predict(c)
            if turn == 0 and c == 0:
                first_sends()

            @pl.when(own == 0)
            def _():
                send_d(turn, 0, c).start()

        def collect_next(stage, c):
            send_d(turn, stage, c).wait_recv()
            sums[turn, stage, c] = sums[turn, stage - 1, c] + got_b[turn, stage - 1, c]
            if stage + 1 < stages:
                send_d(turn, stage + 1, c).start()

        def obtain(c):
            lane = chunk_of(c)

            @pl.when(own == 1)
            def _():
                if stages > 1:
                    collect_next(stages - 1, c)
                send_d(turn, stages, c).start()
                res[:, :, :, lane] = vis[:, :, :, lane] - sums[turn, stages - 1, c]

            @pl.when(own == 0)
            def _():
                send_d(turn, stages, c).wait_recv()
                res[:, :, :, lane] = vis[:, :, :, lane] - got_c[turn, c]

        def gram_of(j):
            m00 = re_mul(j[0], conj(j[0])) + re_mul(j[2], conj(j[2]))
            m11 = re_mul(j[1], conj(j[1])) + re_mul(j[3], conj(j[3]))
            m01 = cadd(cmul_conj(j[1], j[0]), cmul_conj(j[3], j[2]))
            return m00, m11, m01

        def ends_of(lane):
            return [(end(v, lane), end(4 + v, lane)) for v in range(4)]

        def normals(c):
            lane = chunk_of(c)

            def gr(a, b):
                return gram(a, b, lane)

            jp, jq = ends_of(first_of(c)), ends_of(second_of(c))
            m00, m11, m01 = gram_of(jq)
            p00, p11, p01 = gram_of(jp)
            n1_00 = m00 * gr(0, 0) + m11 * gr(1, 1) + 2.0 * re_mul(m01, gr(0, 1))
            n1_11 = m00 * gr(2, 2) + m11 * gr(3, 3) + 2.0 * re_mul(m01, gr(2, 3))
            n1_01 = cadd(
                cadd(scale(m00, gr(0, 2)), scale(m11, gr(1, 3))),
                cadd(cmul(m01, gr(0, 3)), cmul(conj(m01), gr(1, 2))),
            )
            n2_00 = p00 * gr(0, 0) + p11 * gr(2, 2) + 2.0 * re_mul(p01, gr(2, 0))
            n2_11 = p00 * gr(1, 1) + p11 * gr(3, 3) + 2.0 * re_mul(p01, gr(3, 1))
            n2_01 = cadd(
                cadd(scale(p00, gr(1, 0)), scale(p11, gr(3, 2))),
                cadd(cmul(p01, gr(3, 0)), cmul(conj(p01), gr(1, 2))),
            )
            for n, (left, right) in enumerate(
                ((n1_00, n2_00), (n1_11, n2_11), (n1_01[0], n2_01[0]), (n1_01[1], n2_01[1]))
            ):
                vals_n[n * dirs : (n + 1) * dirs, first_of(c)] = left
                vals_n[n * dirs : (n + 1) * dirs, second_of(c)] = right

        def scatter_normals():
            split_store(lhs_n, 4 * dirs, vals_n[...])
            out = join(jnp.dot(lhs_n[...], scatter_hot[...], preferred_element_type=f32), 4 * dirs)
            for g in range(4 * dirs // SUB):
                for j in range(per):
                    seg_n[pl.ds(g * SUB * per + j, SUB, stride=per), :] = out[
                        g * SUB : (g + 1) * SUB, j * LANES : (j + 1) * LANES
                    ]

        def finish(c):
            lane = chunk_of(c)
            r = [[res[v // 4, v % 4, h * SUB : (h + 1) * SUB, lane] for h in range(halves)] for v in range(8)]
            for k in range(dirs):
                co = [[coh[k, v, h * SUB : (h + 1) * SUB, lane] for h in range(halves)] for v in range(8)]
                for a in range(4):
                    for b in range(4):
                        real = sum(r[a][h] * co[b][h] + r[4 + a][h] * co[4 + b][h] for h in range(halves))
                        imag = sum(r[4 + a][h] * co[b][h] - r[a][h] * co[4 + b][h] for h in range(halves))
                        n = 2 * (4 * a + b)
                        cross[n * dirs + k : n * dirs + k + 1, lane] = jnp.sum(real, axis=0, keepdims=True)
                        cross[(n + 1) * dirs + k : (n + 1) * dirs + k + 1, lane] = jnp.sum(
                            imag, axis=0, keepdims=True
                        )

            def crossed(a, b):
                n = 2 * (4 * a + b)
                return (
                    cross[n * dirs : (n + 1) * dirs, lane],
                    cross[(n + 1) * dirs : (n + 2) * dirs, lane],
                )

            jp, jq = ends_of(first_of(c)), ends_of(second_of(c))
            for which, j, other_end in ((0, jq, jp), (1, jp, jq)):
                where = second_of(c) if which else first_of(c)
                h00, h11, re01, im01 = [vals_n[n * dirs : (n + 1) * dirs, where] for n in range(4)]
                h01 = (re01, im01)
                for a in range(2):
                    for d in range(2):
                        total = None
                        for b in range(2):
                            for e in range(2):
                                if which == 0:
                                    term = cmul(j[2 * b + e], crossed(2 * a + b, 2 * d + e))
                                else:
                                    term = cmul_conj(j[2 * b + e], crossed(2 * b + a, 2 * e + d))
                                total = term if total is None else cadd(total, term)
                        if d == 0:
                            extra = cadd(scale(h00, other_end[2 * a]), cmul_conj(other_end[2 * a + 1], h01))
                        else:
                            extra = cadd(cmul(other_end[2 * a], h01), scale(h11, other_end[2 * a + 1]))
                        total = cadd(total, extra)
                        for part in range(2):
                            n = 4 * part + 2 * a + d
                            vals[n * dirs : (n + 1) * dirs, which * LANES : (which + 1) * LANES] = total[part]

            split_store(lhs_c, nrow, vals[...])
            rows = slice(2 * c * LANES, (2 * c + 2) * LANES)
            out = join(jnp.dot(lhs_c[...], scatter_hot[rows, :], preferred_element_type=f32), nrow)
            if c > 0:
                out = out + found[...]
            if c + 1 < chunks:
                found[...] = out
            else:
                for g in range(nrow // SUB):
                    for j in range(per):
                        seg[pl.ds(g * SUB * per + j, SUB, stride=per), :] = out[
                            g * SUB : (g + 1) * SUB, j * LANES : (j + 1) * LANES
                        ]

        if turn == 0:
            collect_all(range(begun, begun + 1))
            lax.fori_loop(0, chunks, gram_body, 0)
        for c in range(chunks):
            normals(c)
        if turn == 0:
            hear(0)
        else:
            scatter_normals()
        collect_all(range(begun + 1 if turn == 0 else 0, chunks))
        if turn == 0:
            scatter_setup()
            start_consensus()
            hear(1)
            loads["vis"].wait()
        if turn > 0 and exchange:

            @pl.when(own == 1)
            def _():
                if turn == 1:
                    solve_weights()
                answer_parts(turn - 1, 1)

            if turn == 2:

                @pl.when(own == 0)
                def _():
                    solve_weights()

        if turn == 1 and not exchange:
            solve_weights()
        if stages > 2:

            @pl.when(own == 1)
            def _():
                for stage in range(1, stages - 1):
                    for c in range(chunks):
                        collect_next(stage, c)

        for c in range(chunks):
            obtain(c)
            if turn > 0 and exchange and c == ANSWER:

                @pl.when(own == 1)
                def _():
                    answer_parts(turn - 1, 0)

            if turn == 0 and c == min(1, chunks - 1):
                scatter_normals()
            finish(c)
            if turn == 0 and c == min(1, chunks - 1):
                for r in range(2, max(2, rounds)):
                    hear(r)
                send_rows()

        def refresh(k, v, total, previous):
            here = packed(k, v)
            fresh = dual[here, :] + RHO * (jones[here, :] - total)
            if previous + 1 < ITERS:
                cons[here, :] = total
                dual[here, :] = fresh
            else:
                dual_out[halves_of(k, v)] = fresh

        def join_parts(previous):
            @pl.when(own == 0)
            def _():
                drain(consin.at[previous], p_recv.at[previous, 2])

            @pl.when(own == 1)
            def _():
                drain(consin.at[previous, pl.ds(1, n_band - 1)], p_recv.at[previous, 2])
                consin[previous, me] = outbox[previous, 1, 0]

            for k in range(dirs):
                for v in range(8):
                    part, rows = part_of(k, v)
                    refresh(k, v, consin[previous, part, rows, :], previous)

        def ring_sum(turn, k, v, slots, total=None):
            for s in slots:
                term = weights[source(s)] * xall[ring(turn), k, s, v]
                total = term if total is None else total + term
            return total

        if turn > 0:
            if exchange:
                join_parts(turn - 1)
            else:
                for s in range(1, ahead + 1):
                    pump(turn - 1, s)
                for k in range(dirs):
                    for v in range(8):
                        refresh(k, v, ring_sum(turn - 1, k, v, range(n_band)), turn - 1)

        by_ring = turn + 1 == ITERS or not exchange
        for k in range(dirs):
            y = []
            for v in range(8):
                here = packed(k, v)
                y.append(seg[here, :] + RHO * cons[here, :] - dual[here, :])
            h00, h11, re01, im01 = [seg_n[packed(k, n), :] for n in range(4)]
            h00 = h00 + RHO
            h11 = h11 + RHO
            inverse = 1.0 / (h00 * h11 - (re01 * re01 + im01 * im01))
            h00, h11, h01 = h00 * inverse, h11 * inverse, (re01 * inverse, im01 * inverse)
            for a in range(2):
                y0, y1 = (y[2 * a], y[4 + 2 * a]), (y[2 * a + 1], y[4 + 2 * a + 1])
                minus0, minus1 = cmul_conj(y1, h01), cmul(y0, h01)
                for part in range(2):
                    for c in range(2):
                        if c == 0:
                            value = h11 * y0[part] - minus0[part]
                        else:
                            value = h00 * y1[part] - minus1[part]
                        v = 4 * part + 2 * a + c
                        here = packed(k, v)
                        jones[here, :] = value
                        if turn + 1 == ITERS:
                            jones_out[halves_of(k, v)] = value
                        sent = value + dual[here, :] * (1.0 / RHO)
                        if by_ring:
                            xall[ring(turn), k, 0, v] = sent
                        else:
                            chunk, rows = part_of(k, v)
                            xs[turn, chunk, rows, :] = sent
        if by_ring:
            for u, way in order:
                if reach_of(u, way):
                    send_x(turn, u, way, 0)
        else:
            send_parts(turn)

    last = ITERS - 1
    for s in range(1, ahead):
        pump(last, s)

    def coeff_body(slots, first):
        def run(m, carry):
            for k in range(dirs):
                total = [None] * 8 if first else [coeffs[(m,) + halves_of(k, v)] for v in range(8)]
                for s in slots:
                    factor = jnp.broadcast_to(gweights[source(s), pl.ds(m, 1), :], (SUB, LANES))
                    for v in range(8):
                        term = factor * xall[ring(last), k, s, v]
                        total[v] = term if total[v] is None else total[v] + term
                for v in range(8):
                    coeffs[(m,) + halves_of(k, v)] = total[v]
            return carry

        lax.fori_loop(0, SUB, run, 0)

    early = range(n_band - 1)
    coeff_body(early, True)
    for k in range(dirs):
        for v in range(8):
            cons[packed(k, v), :] = ring_sum(last, k, v, early)
    pump(last, ahead)
    late = range(n_band - 1, n_band)
    for k in range(dirs):
        for v in range(8):
            refresh(k, v, ring_sum(last, k, v, late, cons[packed(k, v), :]), last)
    coeff_body(late, False)

    drain(rows_all.at[pl.ds(1, n_band - 1)], row_send.at[0])
    drain(xall.at[:, :, pl.ds(1, n_band - 1)], x_send.at[0])

    @pl.when(own == 0)
    def _():
        drain(model, d_send.at[0])
        if exchange:
            drain(xs, p_send.at[0])

    @pl.when(own == 1)
    def _():
        for n in range(1, stages + 1):
            drain(model, d_send.at[n])
        if exchange:
            drain(inbox.at[:, 1, pl.ds(1, n_band - 1)], p_send.at[0])
            drain(inbox.at[:, 0], p_send.at[1])
            drain(inbox.at[:, 1, pl.ds(1, n_band - 1)], p_send.at[1])


def flush(*refs):
    count = (len(refs) - 1) // 2
    sem = refs[-1]
    copies = [pltpu.make_async_copy(refs[n], refs[count + n], sem.at[n]) for n in range(count)]
    for copy in copies:
        copy.start()
    for copy in copies:
        copy.wait()


def power_of_two(n):
    return n & (n - 1) == 0


def ring_cuts(exchange):
    return 2 if exchange else 1


def by_chunks(n_band, rows):
    return power_of_two(n_band) and rows % (n_band * SUB) == 0


def local(n_band, n_dir, vis, coh, jones_start, dual_start, consensus_start, freq_basis, pairs):
    f32 = jnp.float32
    dirs, times, base = coh.shape[1], coh.shape[-2], coh.shape[-1]
    stations = jones_start.shape[-1]
    per = stations // LANES
    nrow = 8 * dirs
    terms = freq_basis.shape[1]

    def enter(value):
        lead = value.shape[:-2]
        value = value.reshape(lead + (2, per, LANES))
        return jnp.swapaxes(value, -2, -3).reshape(lead + (2 * per, LANES))

    def leave(value, shape):
        value = value.reshape(value.shape[:-2] + (per, 2, LANES))
        return jnp.swapaxes(value, -2, -3).reshape(shape)

    stages = n_dir.bit_length() - 1
    chunks = base // LANES
    exchange = by_chunks(n_band, nrow * per)
    rings = 1 if exchange else ITERS
    parts = (ITERS - 1, n_band, max(SUB, nrow * per // n_band), LANES) if exchange else (1, 1, SUB, LANES)
    half = (4, times, base)
    piece = (2, 4, times, LANES)
    vmem = pl.BlockSpec(memory_space=pltpu.VMEM)
    far = pl.BlockSpec(memory_space=pltpu.HBM)
    raw = (dirs, 4, 2 * per, LANES)
    raw_out = jax.ShapeDtypeStruct(raw, f32)
    raw_terms = jax.ShapeDtypeStruct((terms,) + raw, f32)
    bf16 = jnp.bfloat16
    operands = (
        vis.reshape((2,) + half),
        coh.reshape(dirs, 8, times, base),
        enter(jones_start.reshape((dirs, 4, 2, stations))),
        enter(dual_start.reshape((dirs, 4, 2, stations))),
        enter(consensus_start.reshape((terms, dirs, 4, 2, stations))),
        freq_basis,
        pairs,
    )
    results = pl.pallas_call(
        functools.partial(kernel, n_band, n_dir, dirs, times, base, stations),
        out_shape=(pltpu.VMEM(raw, f32), pltpu.VMEM(raw, f32), pltpu.VMEM((terms,) + raw, f32)),
        in_specs=[far] * 7,
        out_specs=(vmem,) * 3,
        scratch_shapes=[
            pltpu.VMEM((2,) + half, f32),
            pltpu.VMEM((dirs, 8, times, base), f32),
            pltpu.VMEM(raw, f32),
            pltpu.VMEM(raw, f32),
            pltpu.VMEM((terms,) + raw, f32),
            pltpu.SMEM(freq_basis.shape, f32),
            pltpu.VMEM((2, base), jnp.int32),
            pltpu.VMEM((nrow * per, LANES), f32),
            pltpu.VMEM((nrow * per, LANES), f32),
            pltpu.VMEM((SUB, LANES), f32),
            pltpu.VMEM((2 * base, LANES), jnp.int32),
            pltpu.VMEM((nrow * per, LANES), f32),
            pltpu.VMEM((rings, dirs, n_band, 8, per, LANES), f32),
            pltpu.VMEM((n_band, SUB, LANES), f32),
            pltpu.VMEM((n_band, SUB, LANES), f32),
            pltpu.VMEM((n_band, SUB, LANES), f32),
            pltpu.VMEM((n_band * n_band if exchange else 1, SUB, LANES), f32),
            pltpu.VMEM(parts, f32),
            pltpu.VMEM(parts[:1] + (2,) + parts[1:], f32),
            pltpu.VMEM(parts[:1] + (2,) + parts[1:], f32),
            pltpu.VMEM(parts, f32),
            pltpu.VMEM((stations, 2 * base), bf16),
            pltpu.VMEM((2 * base, stations), bf16),
            pltpu.VMEM((PIECES * nrow, stations), bf16),
            pltpu.VMEM((PIECES * nrow, 2 * LANES), bf16),
            pltpu.VMEM((PIECES * 4 * dirs, 2 * base), bf16),
            pltpu.VMEM((nrow, 2 * base), f32),
            pltpu.VMEM((20 * dirs, base), f32),
            pltpu.VMEM((32 * dirs, base), f32),
            pltpu.VMEM((nrow, 2 * LANES), f32),
            pltpu.VMEM((4 * dirs, 2 * base), f32),
            pltpu.VMEM((nrow, stations), f32),
            pltpu.VMEM((nrow * per, LANES), f32),
            pltpu.VMEM((4 * dirs * per, LANES), f32),
            pltpu.VMEM((ITERS, chunks) + piece, f32),
            pltpu.VMEM((ITERS, chunks) + piece, f32),
            pltpu.VMEM((ITERS, stages, chunks) + piece, f32),
            pltpu.VMEM((ITERS, max(1, stages - 1), chunks) + piece, f32),
            pltpu.VMEM((ITERS, chunks) + piece, f32),
            pltpu.VMEM((2,) + half, f32),
            pltpu.SemaphoreType.REGULAR((max(1, n_band // 2 - 1) if exchange else 1,)),
            pltpu.SemaphoreType.DMA((6 + chunks,)),
            pltpu.SemaphoreType.DMA((1,)),
            pltpu.SemaphoreType.DMA((1,)),
            pltpu.SemaphoreType.DMA((2,)),
            pltpu.SemaphoreType.DMA((ITERS - 1, 3)),
            pltpu.SemaphoreType.DMA((1,)),
            pltpu.SemaphoreType.DMA((rings, dirs * ring_cuts(exchange), max(1, n_band - 3) if exchange else n_band - 1)),
            pltpu.SemaphoreType.DMA((4,)),
            pltpu.SemaphoreType.DMA((stages + 1,)),
            pltpu.SemaphoreType.DMA((2 * stages - 1, chunks)),
        ],
        compiler_params=pltpu.CompilerParams(
            collective_id=0, has_side_effects=True, vmem_limit_bytes=56 * 1024 * 1024
        ),
    )(*[pltpu.with_memory_space_constraint(x, pltpu.HBM) for x in operands])
    jones, dual, coeffs = pl.pallas_call(
        flush,
        out_shape=(raw_out, raw_out, raw_terms),
        in_specs=[vmem] * 3,
        out_specs=(pl.BlockSpec(memory_space=pltpu.HBM),) * 3,
        scratch_shapes=[pltpu.SemaphoreType.DMA((3,))],
        compiler_params=pltpu.CompilerParams(vmem_limit_bytes=1024 * 1024),
    )(*[pltpu.with_memory_space_constraint(x, pltpu.VMEM) for x in results])
    return (
        leave(jones, jones_start.shape),
        leave(dual, jones_start.shape),
        leave(coeffs, consensus_start.shape),
    )


def solution(mesh):
    in_specs = (
        P("band", None, None, None, None, None),
        P("band", "dir", None, None, None, None, None),
        P("band", "dir", None, None, None, None),
        P("band", "dir", None, None, None, None),
        P(None, "dir", None, None, None, None),
        P("band", None),
        P(),
    )
    out_specs = (
        P("band", "dir", None, None, None, None),
        P("band", "dir", None, None, None, None),
        P(None, "dir", None, None, None, None),
    )
    body = functools.partial(local, mesh.shape["band"], mesh.shape["dir"])
    return jax.shard_map(body, mesh=mesh, in_specs=in_specs, out_specs=out_specs, check_vma=False)
```
